8 devices in a mesh: dp: 1 (over z), tp: 8 (over y, x, core).
Axes of the slice: x: 2, y: 2, z: 1, core: 2. Of those that a mesh axis runs over, the one named last changes fastest.
Arguments:
- x: bfloat16 [1, 2048, 2048], P('dp', 'tp')
- ln1_gamma: float32 [2048], replicated
- ln1_beta: float32 [2048], replicated
- w_qkv: bfloat16 [2048, 16, 3, 128], P(None, 'tp')
- b_qkv: float32 [16, 3, 128], P('tp')
- w_out: bfloat16 [2048, 2048], P('tp')
- b_out: float32 [2048], replicated
- ln2_gamma: float32 [2048], replicated
- ln2_beta: float32 [2048], replicated
- w_up: bfloat16 [2048, 8192], P(None, 'tp')
- b_up: float32 [8192], P('tp')
- w_down: bfloat16 [8192, 2048], P('tp')
- b_down: float32 [2048], replicated
- grad_y: bfloat16 [1, 2048, 2048], P('dp', 'tp')
Outputs:
- output 1: bfloat16 [1, 2048, 2048], P('dp', 'tp')
- output 2: bfloat16 [1, 2048, 2048], P('dp', 'tp')
- output 3: float32 [2048], P('dp')
- output 4: float32 [2048], P('dp')
- output 5: bfloat16 [2048, 16, 3, 128], P('dp', 'tp')
- output 6: float32 [16, 3, 128], P(('dp', 'tp'))
- output 7: bfloat16 [2048, 2048], P(('dp', 'tp'))
- output 8: float32 [2048], P('dp')
- output 9: float32 [2048], P('dp')
- output 10: float32 [2048], P('dp')
- output 11: bfloat16 [2048, 8192], P('dp', 'tp')
- output 12: float32 [8192], P(('dp', 'tp'))
- output 13: bfloat16 [8192, 2048], P(('dp', 'tp'))
- output 14: float32 [2048], P('dp')
All inputs are finite; a program needn't handle non-finite values.
Results may differ from the reference program's by a relative error of at most 0.02.
Values are sent between devices in bfloat16 or wider.
A program may use at most 1 GiB of HBM per device.

```python
import math
import jax
import jax.numpy as jnp
from jax import lax

BATCH = 1
SEQ = 2048
D = 2048
HEADS = 16
HEAD = 128
FF = 8192
EPS = 1e-5
MASK_VALUE = -1e30


def alibi_slopes(n_heads):
    closest = 2 ** int(math.floor(math.log2(n_heads)))
    base_ratio = 2.0 ** (-8.0 / closest)
    extra_ratio = 2.0 ** (-4.0 / closest)
    remaining = min(closest, n_heads - closest)
    slopes = [base_ratio ** (i + 1) for i in range(closest)]
    slopes = slopes + [extra_ratio ** (2 * i + 1) for i in range(remaining)]
    return jnp.array(slopes, dtype=jnp.float32)


def layer_norm(values, ln_gain, ln_bias):
    row_mean = jnp.mean(values, axis=-1, keepdims=True)
    centered = values - row_mean
    variance = jnp.mean(centered * centered, axis=-1, keepdims=True)
    return centered * lax.rsqrt(variance + EPS) * ln_gain + ln_bias


def layer_forward(x, ln1_gamma, ln1_beta, w_qkv, b_qkv, w_out, b_out, ln2_gamma, ln2_beta, w_up, b_up, w_down, b_down):
    positions = jnp.arange(SEQ)
    causal = positions[None, :] <= positions[:, None]
    key_pos = positions.astype(jnp.float32)
    x_f = x.astype(jnp.float32)
    h_norm = layer_norm(x_f, ln1_gamma, ln1_beta).astype(jnp.bfloat16)
    qkv_vals = (jnp.einsum('bsd,dhte->bshte', h_norm.astype(jnp.float32), w_qkv.astype(jnp.float32)) + b_qkv).astype(jnp.bfloat16)
    per_head = jnp.moveaxis(qkv_vals, 2, 0)

    def head_attention(operands):
        head_qkv, head_slope = operands
        q_one = head_qkv[:, :, 0].astype(jnp.float32)
        k_one = head_qkv[:, :, 1].astype(jnp.float32)
        v_one = head_qkv[:, :, 2].astype(jnp.float32)
        scores = jnp.einsum('bie,bje->bij', q_one, k_one) * (HEAD ** -0.5) + head_slope * key_pos
        scores = jnp.where(causal, scores, MASK_VALUE)
        prob_bf = jax.nn.softmax(scores, axis=-1).astype(jnp.bfloat16)
        return jnp.einsum('bij,bje->bie', prob_bf.astype(jnp.float32), v_one).astype(jnp.bfloat16)

    context = lax.map(jax.checkpoint(head_attention), (per_head, alibi_slopes(HEADS)))
    context_flat = jnp.moveaxis(context, 0, 2).reshape(BATCH, SEQ, D)
    attn_out = jnp.einsum('bsc,cd->bsd', context_flat.astype(jnp.float32), w_out.astype(jnp.float32)).astype(jnp.bfloat16)
    x_mid = x_f + attn_out.astype(jnp.float32) + b_out
    g_norm = layer_norm(x_mid, ln2_gamma, ln2_beta).astype(jnp.bfloat16)
    pre_act = jnp.einsum('bsd,df->bsf', g_norm.astype(jnp.float32), w_up.astype(jnp.float32)) + b_up
    activated = jax.nn.gelu(pre_act, approximate=True).astype(jnp.bfloat16)
    mlp_out = jnp.einsum('bsf,fd->bsd', activated.astype(jnp.float32), w_down.astype(jnp.float32)).astype(jnp.bfloat16)
    return (x_mid + mlp_out.astype(jnp.float32) + b_down).astype(jnp.bfloat16)


def setup_inputs(seed: int = 0, part: int = 0) -> dict:
    key_list = jax.random.split(jax.random.key(seed), 14)

    def normal(rng_key, out_shape, std_dev):
        return std_dev * jax.random.normal(rng_key, out_shape, jnp.float32)

    return {
        'x': normal(jax.random.fold_in(key_list[0], part), (BATCH, SEQ, D), 1.0).astype(jnp.bfloat16),
        'ln1_gamma': 1.0 + normal(key_list[1], (D,), 0.2),
        'ln1_beta': normal(key_list[2], (D,), 0.2),
        'w_qkv': normal(key_list[3], (D, HEADS, 3, HEAD), D ** -0.5).astype(jnp.bfloat16),
        'b_qkv': normal(key_list[4], (HEADS, 3, HEAD), 0.5),
        'w_out': normal(key_list[5], (D, D), D ** -0.5).astype(jnp.bfloat16),
        'b_out': normal(key_list[6], (D,), 0.5),
        'ln2_gamma': 1.0 + normal(key_list[7], (D,), 0.2),
        'ln2_beta': normal(key_list[8], (D,), 0.2),
        'w_up': normal(key_list[9], (D, FF), D ** -0.5).astype(jnp.bfloat16),
        'b_up': normal(key_list[10], (FF,), 0.5),
        'w_down': normal(key_list[11], (FF, D), FF ** -0.5).astype(jnp.bfloat16),
        'b_down': normal(key_list[12], (D,), 0.5),
        'grad_y': normal(jax.random.fold_in(key_list[13], part), (BATCH, SEQ, D), 1.0).astype(jnp.bfloat16),
    }


def reference(x, ln1_gamma, ln1_beta, w_qkv, b_qkv, w_out, b_out, ln2_gamma, ln2_beta, w_up, b_up, w_down, b_down, grad_y):
    y, pullback = jax.vjp(layer_forward, x, ln1_gamma, ln1_beta, w_qkv, b_qkv, w_out, b_out, ln2_gamma, ln2_beta, w_up, b_up, w_down, b_down)
    (grad_x, grad_ln1_gamma, grad_ln1_beta, grad_w_qkv, grad_b_qkv, grad_w_out, grad_b_out,
     grad_ln2_gamma, grad_ln2_beta, grad_w_up, grad_b_up, grad_w_down, grad_b_down) = pullback(grad_y)
    return (y, grad_x, grad_ln1_gamma, grad_ln1_beta, grad_w_qkv, grad_b_qkv, grad_w_out, grad_b_out,
            grad_ln2_gamma, grad_ln2_beta, grad_w_up, grad_b_up, grad_w_down, grad_b_down)
```

```python
import functools
import math
import jax
import jax.numpy as jnp
from jax import lax
from jax.experimental import pallas as pl
from jax.experimental.pallas import tpu as pltpu
from jax.sharding import PartitionSpec as P

EPS = 1e-5
MASK_VALUE = -1e30
LOG2E = math.log2(math.e)
MESH = pl.DeviceIdType.MESH
BF = jnp.bfloat16
F32 = jnp.float32
ROWS = 256
CHIP = 512
SEQ = 2048
D = 2048
TN = 512


def alibi_slopes(n_heads):
    closest = 2 ** int(math.floor(math.log2(n_heads)))
    base_ratio = 2.0 ** (-8.0 / closest)
    extra_ratio = 2.0 ** (-4.0 / closest)
    remaining = min(closest, n_heads - closest)
    slopes = [base_ratio ** (i + 1) for i in range(closest)]
    slopes = slopes + [extra_ratio ** (2 * i + 1) for i in range(remaining)]
    return jnp.array(slopes, dtype=jnp.float32)


def dot(a, b):
    return lax.dot_general(a, b, (((1,), (0,)), ((), ())), preferred_element_type=F32)


def dot_nt(a, b):
    return lax.dot_general(a, b, (((1,), (1,)), ((), ())), preferred_element_type=F32)


def dot_tn(a, b):
    return lax.dot_general(a, b, (((0,), (0,)), ((), ())), preferred_element_type=F32)


def places():
    me = lax.axis_index('tp')
    c = lax.rem(me, 2)
    delta = 1 - 2 * c
    xn = me + 2 - 4 * lax.rem(me // 2, 2)
    dy = 4 - 8 * (me // 4)
    return me, me + delta, xn, me + dy, xn + dy, delta


def entry_barrier(peers):
    sem = pltpu.get_barrier_semaphore()
    for p in peers:
        pl.semaphore_signal(sem, inc=1, device_id={'tp': p}, device_id_type=MESH)
    pl.semaphore_wait(sem, len(peers))


def rows_at(block, half=None):
    if half is None:
        return pl.ds(pl.multiple_of(block * ROWS, ROWS), ROWS)
    return pl.ds(pl.multiple_of(block * ROWS + half * 128, 128), 128)


def loop(lo, hi, fn):
    def body(i, carry):
        fn(i)
        return carry
    lax.fori_loop(lo, hi, body, 0)


class Gather:
    def __init__(self, full, ss, rs):
        self.full, self.ss, self.rs = full, ss, rs
        self.me, self.core, self.xn, self.yn, self.dg, delta = places()
        me, core, xn, yn, dg = self.me, self.core, self.xn, self.yn, self.dg
        cx, cy, cd = xn + delta, yn + delta, dg + delta
        self.send_rows = [(me, 0), (me, 1), (yn, 1), (me, 1), (me, 0), (xn, 0), (me, None),
                          (xn, 0), (xn, 1), (yn, 1), (yn, 0), (dg, 0), (dg, 1)]
        self.recv_rows = [(xn, 0), (xn, 1), (dg, 1), (yn, 1), (yn, 0), (dg, 0), (core, None),
                          (cx, 0), (cx, 1), (cy, 1), (cy, 0), (cd, 0), (cd, 1)]
        self.peer = [xn] * 3 + [yn] * 3 + [core] * 7

    def copy(self, k, rows):
        ref = self.full.at[rows_at(*rows)]
        return pltpu.make_async_remote_copy(src_ref=ref, dst_ref=ref, send_sem=self.ss.at[k], recv_sem=self.rs.at[k],
                                            device_id={'tp': self.peer[k]}, device_id_type=MESH)

    def barrier(self):
        entry_barrier([self.core, self.xn, self.yn])

    def send(self, k):
        self.copy(k, self.send_rows[k]).start()

    def recv(self, k):
        self.copy(k, self.recv_rows[k]).wait_recv()

    def run(self, compute, pre=None, landed=None):
        def chip(block):
            return pl.multiple_of((block // 2) * CHIP, CHIP)
        for k in (0, 3, 1, 4, 6):
            self.send(k)
        if pre is not None:
            pre()
        self.recv(6)
        compute(0, chip(self.me))
        self.recv(0)
        self.send(5)
        self.send(7)
        self.recv(3)
        self.send(2)
        self.send(9)
        self.recv(1)
        self.send(8)
        self.recv(4)
        self.send(10)
        self.recv(7)
        self.recv(8)
        compute(1, chip(self.xn))
        self.recv(9)
        self.recv(10)
        compute(2, chip(self.yn))
        self.recv(5)
        self.send(11)
        self.recv(2)
        self.send(12)
        if landed is not None:
            landed()
        self.recv(11)
        self.recv(12)
        compute(3, chip(self.dg))
        for k in range(13):
            self.copy(k, self.send_rows[k]).wait_send()


GATHER_SCRATCH = [pltpu.VMEM((SEQ, D), BF), pltpu.SemaphoreType.DMA((13,)), pltpu.SemaphoreType.DMA((13,))]


class Scatter:
    def __init__(self, pb, din, rel, fin, ss, rs):
        self.pb, self.din, self.rel, self.fin, self.ss, self.rs = pb, din, rel, fin, ss, rs
        self.me, self.core, self.xn, self.yn, dg, self.delta = places()
        self.block = [dg, self.xn, self.yn, self.me]

    def barrier(self):
        entry_barrier([self.core, self.xn, self.yn])

    def copy(self, k):
        lo, hi = pl.ds(0, 128), pl.ds(128, 128)
        din, rel, fin, xn, yn = self.din, self.rel, self.fin, self.xn, self.yn
        if not isinstance(k, int) or k < 4:
            src, dst, peer = self.pb.at[k], din.at[k], self.core
        else:
            src, dst, peer = ((din.at[0, lo], rel.at[0], xn), (din.at[1, lo], fin.at[0, lo], xn), (din.at[1, hi], fin.at[0, hi], xn),
                              (din.at[0, hi], rel.at[1], yn), (din.at[2, hi], fin.at[1, hi], yn), (din.at[2, lo], fin.at[1, lo], yn))[k - 4]
        return pltpu.make_async_remote_copy(src_ref=src, dst_ref=dst, send_sem=self.ss.at[k], recv_sem=self.rs.at[k],
                                            device_id={'tp': peer}, device_id_type=MESH)

    def give(self, d, tile, block=None):
        block = self.block[d] + self.delta if block is None else block
        def body(n):
            cols = pl.ds(pl.multiple_of(n * TN, TN), TN)
            self.pb[d, :, cols] = tile(block, n).astype(BF)
        loop(0, D // TN, body)
        self.copy(d).start()

    def keep(self, d, tile):
        self.copy(d).wait_recv()
        def body(n):
            cols = pl.ds(pl.multiple_of(n * TN, TN), TN)
            self.din[d, :, cols] = (tile(self.block[d], n) + self.din[d, :, cols].astype(F32)).astype(BF)
        loop(0, D // TN, body)

    def start(self, *flows):
        for k in flows:
            self.copy(k).start()

    def add_relay(self, d, half, slot):
        def body(n):
            rows = pl.ds(pl.multiple_of(half * 128 + n * 16, 16), 16)
            src = pl.ds(pl.multiple_of(n * 16, 16), 16)
            self.din[d, rows] = (self.din[d, rows].astype(F32) + self.rel[slot, src].astype(F32)).astype(BF)
        loop(0, 8, body)

    def relays(self):
        self.copy(4).wait_recv()
        self.add_relay(2, 0, 0)
        self.start(9)
        self.copy(7).wait_recv()
        self.add_relay(1, 1, 1)
        self.start(6)

    def arrive(self):
        for k in (5, 8, 6, 9):
            self.copy(k).wait_recv()

    def run(self, tile):
        self.give(0, tile)
        self.give(1, tile)
        self.keep(0, tile)
        self.start(4, 7)
        self.give(2, tile)
        self.keep(1, tile)
        self.start(5)
        self.give(3, tile)
        self.keep(2, tile)
        self.start(8)
        self.keep(3, tile)

    def total(self, rows):
        s = self.din[3, rows].astype(F32) + self.fin[0, rows].astype(F32) + self.fin[1, rows].astype(F32)
        return s.astype(BF).astype(F32)

    def finish(self, first=0):
        for k in range(first, 10):
            self.copy(k).wait_send()


SCATTER_REST = [pltpu.VMEM((4, ROWS, D), BF), pltpu.VMEM((2, 128, D), BF), pltpu.VMEM((2, ROWS, D), BF),
                pltpu.SemaphoreType.DMA((10,)), pltpu.SemaphoreType.DMA((10,))]
SCATTER_SCRATCH = [pltpu.VMEM((4, ROWS, D), BF)] + SCATTER_REST
VM = pl.BlockSpec(memory_space=pltpu.VMEM)
HB = pl.BlockSpec(memory_space=pl.ANY)


def call(body, name, cid, ins, outs, scratch, args, flops):
    return pl.pallas_call(
        body,
        name=name,
        out_shape=[jax.ShapeDtypeStruct(s, t) for s, t, _ in outs],
        in_specs=ins,
        out_specs=[m for _, _, m in outs],
        scratch_shapes=scratch,
        compiler_params=pltpu.CompilerParams(collective_id=cid, has_side_effects=True, vmem_limit_bytes=67043328),
        cost_estimate=pl.CostEstimate(flops=flops, bytes_accessed=32 << 20, transcendentals=0),
    )(*args)


def norm_rows(v, gain, bias):
    mean = jnp.mean(v, axis=-1, keepdims=True)
    cent = v - mean
    var = jnp.mean(cent * cent, axis=-1, keepdims=True)
    return cent * lax.rsqrt(var + EPS) * gain + bias


def norm_rows_back(v, gain, ct):
    mean = jnp.mean(v, axis=-1, keepdims=True)
    cent = v - mean
    rstd = lax.rsqrt(jnp.mean(cent * cent, axis=-1, keepdims=True) + EPS)
    xhat = cent * rstd
    gx = ct * gain
    m1 = jnp.mean(gx, axis=-1, keepdims=True)
    m2 = jnp.mean(gx * xhat, axis=-1, keepdims=True)
    return rstd * (gx - m1 - xhat * m2), xhat


RB = 32


def row_blocks(fn):
    loop(0, ROWS // RB, lambda i: fn(pl.ds(pl.multiple_of(i * RB, RB), RB)))


def front_kernel(sl_ref, x_hbm, g1_ref, b1_ref, w6_hbm, bq_ref, gyl_hbm, wo_hbm, bo_ref, g2_ref, b2_ref,
                 qkv_out, ctx_out, lse_ref, h_out, gy_out, x1_ref, gl_ref,
                 full, ss, rs, gyf, ssy, rsy, x, w6, wo, qkv, ctx, bias, biasm, acc, ml, ls, hs, ys, *scratch):
    ag = Gather(full, ss, rs)
    gg = Gather(gyf, ssy, rsy)
    sc = Scatter(*scratch)
    pairs = [(x_hbm, x), (gyl_hbm, gyf.at[rows_at(ag.me)]), (w6_hbm, w6), (wo_hbm, wo)]
    loads = [pltpu.make_async_copy(src, dst, ls.at[i]) for i, (src, dst) in enumerate(pairs)]
    for l in loads:
        l.start()
    loads[0].wait()

    def ln(i):
        rows = pl.ds(pl.multiple_of(i * RB, RB), RB)
        dst = pl.ds(pl.multiple_of(ag.me * ROWS + i * RB, RB), RB)
        full[dst] = norm_rows(x[rows].astype(F32), g1_ref[...], b1_ref[...]).astype(BF)
    loop(0, ROWS // RB, ln)
    ag.barrier()
    c1 = (128 ** -0.5) * LOG2E

    def biases():
        ki = lax.broadcasted_iota(jnp.int32, (CHIP, CHIP), 0)
        qi = lax.broadcasted_iota(jnp.int32, (CHIP, CHIP), 1)
        for h in range(2):
            b = ki.astype(F32) * (sl_ref[h] * LOG2E)
            bias[h] = b
            biasm[h] = jnp.where(ki <= qi, b, MASK_VALUE)
        for l in loads[1:]:
            l.wait()

    def compute(idx, r0):
        rows = pl.ds(r0, CHIP)
        pltpu.make_async_copy(full.at[rows], h_out.at[rows], hs.at[idx]).start()
        def body(t):
            cols = pl.ds(pl.multiple_of(t * 256, 256), 256)
            w = jnp.concatenate([w6[2 * t], w6[2 * t + 1]], axis=1)
            qkv[rows, cols] = (dot(full[rows], w) + bq_ref[:, cols]).astype(BF)
        loop(0, 3, body)

    def start_gy():
        for k in (0, 3, 1, 4, 6):
            gg.send(k)
    ag.run(compute, pre=biases, landed=start_gy)
    stores = [pltpu.make_async_copy(qkv, qkv_out, ls.at[4]), pltpu.make_async_copy(ctx, ctx_out, ls.at[5])]
    stores[0].start()

    def tile(block, n):
        cols = pl.ds(pl.multiple_of(n * TN, TN), TN)
        return dot(ctx[rows_at(block)], wo[:, cols])

    xb = lax.rem(ag.me // 2, 2)
    yb = ag.me // 4

    def attend(p):
        nx = xb + (1 - p // 2) * (1 - 2 * xb)
        ny = yb + (1 - lax.rem(p, 2)) * (1 - 2 * yb)
        i = 2 * ny + nx
        qrows = pl.ds(pl.multiple_of(i * CHIP, CHIP), CHIP)

        def one(h):
            lanes = [pl.ds(pl.multiple_of((2 * t + h) * 128, 128), 128) for t in range(3)]
            sl = sl_ref[h] * LOG2E
            q = qkv[qrows, lanes[0]]
            ml[0:1] = jnp.full((1, CHIP), MASK_VALUE, F32)
            ml[1:2] = jnp.zeros((1, CHIP), F32)
            acc[...] = jnp.zeros_like(acc)
            def step(j, bias_ref):
                krows = pl.ds(pl.multiple_of(j * CHIP, CHIP), CHIP)
                s = dot_nt(qkv[krows, lanes[1]], q) * c1 + bias_ref[h]
                cj = sl * (j * CHIP).astype(F32)
                m = ml[0:1]
                mn = jnp.maximum(m, jnp.max(s, axis=0, keepdims=True) + cj)
                pr = jnp.exp2(s - (mn - cj))
                alpha = jnp.exp2(m - mn)
                ml[1:2] = ml[1:2] * alpha + jnp.sum(pr, axis=0, keepdims=True)
                ml[0:1] = mn
                acc[...] = acc[...] * alpha + dot_tn(qkv[krows, lanes[2]], pr.astype(BF))
            loop(0, i, lambda j: step(j, bias))
            step(i, biasm)
            ctx[qrows, lanes[0]] = jnp.transpose(acc[...] / ml[1:2]).astype(BF)
            lse_ref[h, :, qrows] = ml[0:1] + jnp.log(ml[1:2]) * LOG2E
        loop(0, 2, one)
        sc.give(p, tile, 2 * i + 1 - lax.rem(ag.me, 2))
    loop(0, 4, attend)
    stores[1].start()

    gg.recv(0)
    gg.send(5)
    gg.send(7)
    gg.recv(3)
    gg.send(2)
    gg.send(9)
    sc.keep(0, tile)
    sc.start(4, 7)
    sc.keep(1, tile)
    sc.start(5)
    sc.keep(2, tile)
    sc.start(8)
    sc.keep(3, tile)
    gg.recv(1)
    gg.send(8)
    gg.recv(4)
    gg.send(10)

    chips = [pl.multiple_of((b // 2) * CHIP, CHIP) for b in (ag.me, ag.xn, ag.yn, ag.dg)]
    def keep_gy(i):
        rows = pl.ds(chips[i], CHIP)
        return pltpu.make_async_copy(gyf.at[rows], gy_out.at[rows], ys.at[i])
    gg.recv(6)
    keep_gy(0).start()
    sc.relays()
    for k in (7, 8):
        gg.recv(k)
    keep_gy(1).start()
    for k in (9, 10):
        gg.recv(k)
    keep_gy(2).start()
    gg.recv(5)
    gg.send(11)
    gg.recv(2)
    gg.send(12)
    sc.arrive()

    def fin(rows):
        x1 = x[rows].astype(F32) + sc.total(rows) + bo_ref[...]
        x1_ref[rows] = x1
        gl_ref[rows] = norm_rows(x1, g2_ref[...], b2_ref[...]).astype(BF)
    row_blocks(fin)
    for k in (11, 12):
        gg.recv(k)
    keep_gy(3).start()
    sc.finish()
    for k in range(13):
        gg.copy(k, gg.send_rows[k]).wait_send()
    for s in stores:
        s.wait()
    for i in range(4):
        rows = pl.ds(i * CHIP, CHIP)
        pltpu.make_async_copy(full.at[rows], h_out.at[rows], hs.at[i]).wait()
        keep_gy(i).wait()


def mlp_kernel(g_hbm, gy_hbm, wu_hbm, bu_ref, wd_hbm, x1_hbm, g2_ref,
               r_out, gm_ref, gmb_ref, vec_ref, gwu_out, gwd_out, gbu_ref, gbd_ref,
               full, ss, rs, gy, wu, wd, x1, gp, r, gw, ls, ys, *scratch):
    ag = Gather(full, ss, rs)
    sc = Scatter(*scratch)
    own = pltpu.make_async_copy(g_hbm, full.at[rows_at(ag.me)], ls.at[0])
    own.start()
    load_wd = pltpu.make_async_copy(wd_hbm, wd, ls.at[1])
    load_wd.start()
    chips = [pl.multiple_of((b // 2) * CHIP, CHIP) for b in (ag.me, ag.xn, ag.yn, ag.dg)]
    load_gy = [pltpu.make_async_copy(gy_hbm.at[pl.ds(c, CHIP)], gy.at[pl.ds(c, CHIP)], ys.at[i]) for i, c in enumerate(chips)]
    for l in load_gy:
        l.start()
    load_wu = pltpu.make_async_copy(wu_hbm, wu, ls.at[2])
    load_wu.start()
    load_x1 = pltpu.make_async_copy(x1_hbm, x1, ls.at[3])
    load_x1.start()
    own.wait()
    ag.barrier()
    for k in (0, 3, 1, 4, 6):
        ag.send(k)
    gbu_ref[...] = jnp.zeros_like(gbu_ref)
    gbd_ref[...] = jnp.zeros_like(gbd_ref)
    vec_ref[...] = jnp.zeros_like(vec_ref)

    def act(i):
        rows = pl.ds(chips[i], CHIP)
        load_gy[i].wait()
        def body(n):
            cols = pl.ds(pl.multiple_of(n * 256, 256), 256)
            gp[rows, cols] = dot_nt(gy[rows], wd[cols]).astype(BF)
        loop(0, 4, body)

    def colsum(n):
        part = pl.ds(pl.multiple_of(n * RB, RB), RB)
        gbd_ref[...] += jnp.sum(gy[part].astype(F32), axis=0, keepdims=True)

    k0 = math.sqrt(2.0 / math.pi)
    k1 = 0.044715

    def up(i):
        rows = pl.ds(chips[i], CHIP)
        def body(n):
            cols = pl.ds(pl.multiple_of(n * 256, 256), 256)
            z = dot(full[rows], wu[:, cols]) + bu_ref[:, cols]
            z2 = z * z
            t = jnp.tanh(k0 * (z + k1 * (z2 * z)))
            half = 0.5 * (1.0 + t)
            r[rows, cols] = (z * half).astype(BF)
            dz = half + (0.5 * z) * (1.0 - t * t) * (k0 * (1.0 + 3.0 * k1 * z2))
            gpre = gp[rows, cols].astype(F32) * dz
            gbu_ref[:, cols] += jnp.sum(gpre, axis=0, keepdims=True)
            gp[rows, cols] = gpre.astype(BF)
        loop(0, 4, body)
        pltpu.make_async_copy(r.at[rows], r_out.at[rows], ys.at[i]).start()

    def tile(block, n):
        cols = pl.ds(pl.multiple_of(n * TN, TN), TN)
        return dot_nt(gp[rows_at(block)], wu[cols])

    load_wd.wait()
    act(0)
    load_wu.wait()
    ag.recv(6)
    up(0)
    act(1)
    ag.recv(0)
    ag.send(5)
    ag.send(7)
    ag.recv(3)
    ag.send(2)
    ag.send(9)
    act(2)
    act(3)
    loop(0, SEQ // RB // 2, colsum)
    ag.recv(1)
    ag.send(8)
    ag.recv(4)
    ag.send(10)
    ag.recv(7)
    ag.recv(8)
    up(1)
    sc.give(1, tile)
    ag.recv(9)
    ag.recv(10)
    up(2)
    sc.give(2, tile)
    ag.recv(5)
    ag.send(11)
    ag.recv(2)
    ag.send(12)
    sc.keep(1, tile)
    sc.start(5)
    sc.keep(2, tile)
    sc.start(8)
    ag.recv(11)
    ag.recv(12)
    up(3)
    sc.give(0, tile)
    sc.give(3, tile)
    sc.keep(0, tile)
    sc.start(4, 7)
    sc.keep(3, tile)

    def gwu_step(i):
        cols = pl.ds(pl.multiple_of(i * 256, 256), 256)
        gw[:, pl.ds(0, 1024)] = dot_tn(full[:, cols], gp[...]).astype(BF)
        c = pltpu.make_async_copy(gw.at[:, pl.ds(0, 1024)], gwu_out.at[cols], ls.at[4])
        c.start()
        c.wait()

    def gwd_step(i):
        cols = pl.ds(pl.multiple_of(i * 256, 256), 256)
        gw[...] = dot_tn(r[:, cols], gy[...]).astype(BF)
        c = pltpu.make_async_copy(gw, gwd_out.at[cols], ls.at[4])
        c.start()
        c.wait()

    loop(0, 6, gwu_step)
    sc.relays()
    loop(6, 8, gwu_step)
    loop(0, 4, gwd_step)
    loop(SEQ // RB // 2, SEQ // RB, colsum)
    load_x1.wait()
    sc.arrive()

    def fin(rows):
        ct = sc.total(rows)
        dx, xhat = norm_rows_back(x1[rows], g2_ref[...], ct)
        mine = pl.ds(pl.multiple_of(ag.me * ROWS + rows.start, RB), RB)
        gm = gy[mine].astype(F32) + dx
        gm_ref[rows] = gm
        gmb_ref[rows] = gm.astype(BF)
        vec_ref[0:1] += jnp.sum(ct * xhat, axis=0, keepdims=True)
        vec_ref[1:2] += jnp.sum(ct, axis=0, keepdims=True)
        vec_ref[2:3] += jnp.sum(gm, axis=0, keepdims=True)
    row_blocks(fin)
    for k in range(13):
        ag.copy(k, ag.send_rows[k]).wait_send()
    sc.finish()
    for i in range(4):
        rows = pl.ds(chips[i], CHIP)
        pltpu.make_async_copy(r.at[rows], r_out.at[rows], ys.at[i]).wait()


def tail_kernel(sl_ref, gm_hbm, wo_hbm, r_hbm, wd_hbm, qkv_hbm, ctx_hbm, lse_ref, w6_hbm, x_hbm, gmf_hbm, x1_hbm, bd_ref, g1_ref,
                h_hbm, vec2_ref, y_ref, gx_ref, vec_out, gwq_out, gwo_out, gb_ref,
                full, ss, rs, wo, r, wd, qkv, ctx, w6, x1, gc, gq, gwq, gwo, bias, biasm, delta, dqt, dk, dv, vec, bufv,
                ls, vs, vr, pb, din1, rel1, fin1, ss1, rs1, din2, rel2, fin2, ss2, rs2):
    ag = Gather(full, ss, rs)
    s1 = Scatter(pb, din1, rel1, fin1, ss1, rs1)
    s2 = Scatter(pb, din2, rel2, fin2, ss2, rs2)
    pairs = [(gm_hbm, full.at[rows_at(ag.me)]), (wd_hbm, wd), (r_hbm, r), (wo_hbm, wo), (qkv_hbm, qkv), (ctx_hbm, ctx), (w6_hbm, w6),
             (x1_hbm, x1)]
    loads = [pltpu.make_async_copy(src, dst, ls.at[i]) for i, (src, dst) in enumerate(pairs)]
    for l in loads:
        l.start()
    loads[0].wait()
    peers = [lax.rem(ag.me + k, 8) for k in range(1, 8)]
    entry_barrier(peers)
    for k in (0, 3, 1, 4, 6):
        ag.send(k)
    scale = 128 ** -0.5
    c1 = scale * LOG2E
    vec[...] = vec2_ref[...]
    gb_ref[...] = jnp.zeros_like(gb_ref)

    def mtile(block, n):
        cols = pl.ds(pl.multiple_of(n * TN, TN), TN)
        return dot(r[rows_at(block)], wd[:, cols])

    def gcs(block):
        rows = pl.ds(pl.multiple_of((block // 2) * CHIP, CHIP), CHIP)
        gc[rows] = dot_nt(full[rows], wo[...]).astype(BF)

    loads[1].wait()
    loads[2].wait()
    for d in range(4):
        s1.give(d, mtile)
    s1.keep(0, mtile)
    loads[3].wait()
    ag.recv(6)
    gcs(ag.me)
    ag.recv(0)
    ag.send(5)
    ag.send(7)
    ag.recv(3)
    ag.send(2)
    ag.send(9)
    for d in range(1, 4):
        s1.keep(d, mtile)
    load_h = [pltpu.make_async_copy(h_hbm.at[:, pl.ds(i * 1024, 1024)], r, ls.at[10 + i]) for i in range(2)]
    load_h[0].start()
    for l in loads[4:]:
        l.wait()

    def rowsum(i):
        rows = pl.ds(pl.multiple_of(i * CHIP, CHIP), CHIP)
        for h in range(2):
            lanes = pl.ds(h * 128, 128)
            prod = gc[rows, lanes].astype(F32) * ctx[rows, lanes].astype(F32)
            delta[h:h + 1, rows] = jnp.sum(jnp.transpose(prod), axis=0, keepdims=True)

    ag.recv(1)
    ag.send(8)
    ag.recv(4)
    ag.send(10)
    ag.recv(7)
    ag.recv(8)
    gcs(ag.xn)
    ag.recv(9)
    ag.recv(10)
    gcs(ag.yn)
    ag.recv(5)
    ag.send(11)
    ag.recv(2)
    ag.send(12)
    s1.start(4, 7, 5, 8)
    ag.recv(11)
    ag.recv(12)
    gcs(ag.dg)
    x = wo
    load_x = pltpu.make_async_copy(x_hbm, x, ls.at[8])
    load_x.start()
    loop(0, SEQ // CHIP, rowsum)

    def put(h, t, rows, val):
        val = val.astype(BF)
        gq[rows, (2 * t + h) * 128:(2 * t + h + 1) * 128] = val
        gb_ref[h, t:t + 1] += jnp.sum(val.astype(F32), axis=0, keepdims=True)

    def head(h):
        sl = sl_ref[h] * LOG2E
        ki = lax.broadcasted_iota(jnp.int32, (CHIP, CHIP), 0)
        qi = lax.broadcasted_iota(jnp.int32, (CHIP, CHIP), 1)
        b = ki.astype(F32) * sl
        bias[...] = b
        biasm[...] = jnp.where(ki <= qi, b, MASK_VALUE)
        dqt[...] = jnp.zeros_like(dqt)
        lq, lk, lv, lo = (pl.ds((2 * t + h) * 128, 128) for t in (0, 1, 2, 0))

        def kblock(j):
            krows = pl.ds(pl.multiple_of(j * CHIP, CHIP), CHIP)
            k = qkv[krows, lk]
            v = qkv[krows, lv]
            dk[...] = jnp.zeros_like(dk)
            dv[...] = jnp.zeros_like(dv)
            cj = sl * (j * CHIP).astype(F32)
            def step(i, bias_ref):
                qrows = pl.ds(pl.multiple_of(i * CHIP, CHIP), CHIP)
                q = qkv[qrows, lq]
                do = gc[qrows, lo]
                p = jnp.exp2(dot_nt(k, q) * c1 + bias_ref[...] - (lse_ref[h, :, qrows] - cj))
                dv[...] += dot(p.astype(BF), do)
                ds = (p * (dot_nt(v, do) - delta[h:h + 1, qrows])).astype(BF)
                dk[...] += dot(ds, q)
                dqt[:, qrows] += dot_tn(k, ds)
            step(j, biasm)
            loop(j + 1, SEQ // CHIP, lambda i: step(i, bias))
            put(h, 1, krows, dk[...] * scale)
            put(h, 2, krows, dv[...])
        loop(0, SEQ // CHIP, kblock)

        def qout(i):
            rows = pl.ds(pl.multiple_of(i * CHIP, CHIP), CHIP)
            put(h, 0, rows, jnp.transpose(dqt[:, rows]) * scale)
        loop(0, SEQ // CHIP, qout)

    head(0)
    s1.relays()
    head(1)

    def htile(block, n):
        rows = rows_at(block)
        cols = pl.ds(pl.multiple_of(n * TN, TN), TN)
        out = None
        for t in range(3):
            w = jnp.concatenate([w6[2 * t, cols], w6[2 * t + 1, cols]], axis=1)
            part = dot_nt(gq[rows, t * 256:(t + 1) * 256], w)
            out = part if out is None else out + part
        return out

    for k in range(4):
        s1.copy(k).wait_send()
    s2.run(htile)

    stores = [pltpu.make_async_copy(gwq, gwq_out.at[pl.ds(i * 1024, 1024)], ls.at[12]) for i in range(2)]
    stores.append(pltpu.make_async_copy(gwo, gwo_out, ls.at[13]))

    def wq():
        def body(i):
            src = pl.ds(pl.multiple_of(i * 256, 256), 256)
            gwq[src] = dot_tn(r[:, src], gq[...]).astype(BF)
        return body

    load_h[0].wait()
    loop(0, 4, wq())
    load_h[1].start()
    stores[0].start()
    s2.relays()
    s1.arrive()

    def yrow(rows):
        y_ref[rows] = (x1[rows] + s1.total(rows) + bd_ref[...]).astype(BF)
    row_blocks(yrow)
    gm = x1
    load_gm = pltpu.make_async_copy(gmf_hbm, gm, ls.at[9])
    load_gm.start()

    def wout(n):
        cols = pl.ds(pl.multiple_of(n * TN, TN), TN)
        gwo[:, cols] = dot_tn(ctx[...], full[:, cols]).astype(BF)
    loop(0, D // TN, wout)
    stores[2].start()
    load_h[1].wait()
    stores[0].wait()
    loop(0, 4, wq())
    stores[1].start()
    load_x.wait()
    load_gm.wait()
    s2.arrive()

    def fin(rows):
        ct = s2.total(rows)
        dx, xhat = norm_rows_back(x[rows].astype(F32), g1_ref[...], ct)
        gx_ref[rows] = (gm[rows] + dx).astype(BF)
        vec[3:4] += jnp.sum(ct * xhat, axis=0, keepdims=True)
        vec[4:5] += jnp.sum(ct, axis=0, keepdims=True)
    row_blocks(fin)
    s1.finish(4)
    s2.finish()
    copies = [pltpu.make_async_remote_copy(src_ref=vec, dst_ref=bufv.at[ag.me], send_sem=vs.at[k], recv_sem=vr.at[k],
                                           device_id={'tp': peers[k]}, device_id_type=MESH) for k in range(7)]
    for c in copies:
        c.start()
    bufv[ag.me] = vec[...]
    for k in range(13):
        ag.copy(k, ag.send_rows[k]).wait_send()
    for s in stores[1:]:
        s.wait()
    for c in copies:
        c.wait()
    total = bufv[0]
    for i in range(1, 8):
        total = total + bufv[i]
    vec_out[...] = total


def solution(mesh):
    def local_step(x, ln1_gamma, ln1_beta, w_qkv, b_qkv, w_out, b_out, ln2_gamma, ln2_beta, w_up, b_up, w_down, b_down, grad_y):
        tp_index = lax.axis_index('tp')
        slopes = lax.dynamic_slice_in_dim(alibi_slopes(16), tp_index * 2, 2)
        row = lambda v: v.reshape(1, -1)
        x2, gy2 = x[0], grad_y[0]
        w6 = w_qkv.transpose(2, 1, 0, 3).reshape(6, D, 128)
        bq = b_qkv.transpose(1, 0, 2).reshape(1, 768)

        qkv, ctx, lse, h_full, gy_full, x1, g_loc = call(
            front_kernel, 'front', 0, [pl.BlockSpec(memory_space=pltpu.SMEM), HB, VM, VM, HB, VM, HB, HB, VM, VM, VM],
            [((SEQ, 768), BF, HB), ((SEQ, 256), BF, HB), ((2, 1, SEQ), F32, VM), ((SEQ, D), BF, HB), ((SEQ, D), BF, HB),
             ((ROWS, D), F32, VM), ((ROWS, D), BF, VM)],
            GATHER_SCRATCH * 2 + [pltpu.VMEM((ROWS, D), BF), pltpu.VMEM((6, D, 128), BF), pltpu.VMEM((256, D), BF),
                                  pltpu.VMEM((SEQ, 768), BF), pltpu.VMEM((SEQ, 256), BF), pltpu.VMEM((2, CHIP, CHIP), F32),
                                  pltpu.VMEM((2, CHIP, CHIP), F32), pltpu.VMEM((128, CHIP), F32), pltpu.VMEM((8, CHIP), F32),
                                  pltpu.SemaphoreType.DMA((6,)), pltpu.SemaphoreType.DMA((4,)), pltpu.SemaphoreType.DMA((4,))]
            + SCATTER_SCRATCH,
            (slopes, x2, row(ln1_gamma), row(ln1_beta), w6, bq, gy2, w_out, row(b_out), row(ln2_gamma), row(ln2_beta)), 12 << 30)
        r, gm, gm_bf, vec2, g_wu, g_wd, gbu, gbd = call(
            mlp_kernel, 'mlp', 2, [HB, HB, HB, VM, HB, HB, VM],
            [((SEQ, 1024), BF, HB), ((ROWS, D), F32, VM), ((ROWS, D), BF, VM), ((8, D), F32, VM), ((D, 1024), BF, HB),
             ((1024, D), BF, HB), ((1, 1024), F32, VM), ((1, D), F32, VM)],
            GATHER_SCRATCH + [pltpu.VMEM((SEQ, D), BF), pltpu.VMEM((D, 1024), BF), pltpu.VMEM((1024, D), BF), pltpu.VMEM((ROWS, D), F32),
                              pltpu.VMEM((SEQ, 1024), BF), pltpu.VMEM((SEQ, 1024), BF), pltpu.VMEM((256, D), BF),
                              pltpu.SemaphoreType.DMA((5,)), pltpu.SemaphoreType.DMA((4,))] + SCATTER_SCRATCH,
            (g_loc, gy_full, w_up, row(b_up), w_down, x1, row(ln2_gamma)), 45 << 30)
        y, g_x, vec, g_wq, g_wo, g_bq = call(
            tail_kernel, 'tail', 3, [pl.BlockSpec(memory_space=pltpu.SMEM)] + [HB] * 6 + [VM] + [HB] * 4 + [VM] * 2 + [HB, VM],
            [((ROWS, D), BF, VM), ((ROWS, D), BF, VM), ((8, D), F32, VM), ((D, 768), BF, HB), ((256, D), BF, HB), ((2, 3, 128), F32, VM)],
            GATHER_SCRATCH + [pltpu.VMEM((256, D), BF), pltpu.VMEM((SEQ, 1024), BF), pltpu.VMEM((1024, D), BF), pltpu.VMEM((SEQ, 768), BF),
                              pltpu.VMEM((SEQ, 256), BF), pltpu.VMEM((6, D, 128), BF), pltpu.VMEM((ROWS, D), F32),
                              pltpu.VMEM((SEQ, 256), BF), pltpu.VMEM((SEQ, 768), BF), pltpu.VMEM((1024, 768), BF),
                              pltpu.VMEM((256, D), BF), pltpu.VMEM((CHIP, CHIP), F32), pltpu.VMEM((CHIP, CHIP), F32),
                              pltpu.VMEM((2, SEQ), F32), pltpu.VMEM((128, SEQ), F32), pltpu.VMEM((CHIP, 128), F32),
                              pltpu.VMEM((CHIP, 128), F32), pltpu.VMEM((8, D), F32), pltpu.VMEM((8, 8, D), F32),
                              pltpu.SemaphoreType.DMA((14,)), pltpu.SemaphoreType.DMA((7,)), pltpu.SemaphoreType.DMA((7,))]
            + SCATTER_SCRATCH + SCATTER_REST,
            (slopes, gm_bf, w_out, r, w_down, qkv, ctx, lse, w6, x2, gm, x1, row(b_down), row(ln1_gamma), h_full, vec2), 55 << 30)
        g_wq = g_wq.reshape(D, 3, 2, 128).transpose(0, 2, 1, 3)
        return (y[None], g_x[None], vec[3], vec[4], g_wq, g_bq, g_wo, vec[2], vec[0], vec[1], g_wu, gbu[0], g_wd, gbd[0])

    row_spec = P('dp', 'tp', None)
    in_specs = (row_spec, P(), P(), P(None, 'tp', None, None), P('tp', None, None), P('tp', None), P(), P(), P(),
                P(None, 'tp'), P('tp'), P('tp', None), P(), row_spec)
    out_specs = (row_spec, row_spec, P('dp'), P('dp'), P('dp', 'tp', None, None), P(('dp', 'tp'), None, None),
                 P(('dp', 'tp'), None), P('dp'), P('dp'), P('dp'), P('dp', 'tp'), P(('dp', 'tp')), P(('dp', 'tp'), None), P('dp'))
    return jax.shard_map(local_step, mesh=mesh, in_specs=in_specs, out_specs=out_specs, check_vma=False)
```

```python
import functools
import math
import jax
import jax.numpy as jnp
from jax import lax
from jax.experimental import pallas as pl
from jax.experimental.pallas import tpu as pltpu
from jax.sharding import PartitionSpec as P

EPS = 1e-5
MASK_VALUE = -1e30
LOG2E = math.log2(math.e)
MESH = pl.DeviceIdType.MESH
BF = jnp.bfloat16
F32 = jnp.float32
ROWS = 256
CHIP = 512
SEQ = 2048
D = 2048
TN = 512


def alibi_slopes(n_heads):
    closest = 2 ** int(math.floor(math.log2(n_heads)))
    base_ratio = 2.0 ** (-8.0 / closest)
    extra_ratio = 2.0 ** (-4.0 / closest)
    remaining = min(closest, n_heads - closest)
    slopes = [base_ratio ** (i + 1) for i in range(closest)]
    slopes = slopes + [extra_ratio ** (2 * i + 1) for i in range(remaining)]
    return jnp.array(slopes, dtype=jnp.float32)


def dot(a, b):
    return lax.dot_general(a, b, (((1,), (0,)), ((), ())), preferred_element_type=F32)


def dot_nt(a, b):
    return lax.dot_general(a, b, (((1,), (1,)), ((), ())), preferred_element_type=F32)


def dot_tn(a, b):
    return lax.dot_general(a, b, (((0,), (0,)), ((), ())), preferred_element_type=F32)


def places():
    me = lax.axis_index('tp')
    c = lax.rem(me, 2)
    delta = 1 - 2 * c
    xn = me + 2 - 4 * lax.rem(me // 2, 2)
    dy = 4 - 8 * (me // 4)
    return me, me + delta, xn, me + dy, xn + dy, delta


def entry_barrier(peers):
    sem = pltpu.get_barrier_semaphore()
    for p in peers:
        pl.semaphore_signal(sem, inc=1, device_id={'tp': p}, device_id_type=MESH)
    pl.semaphore_wait(sem, len(peers))


def rows_at(block, half=None):
    if half is None:
        return pl.ds(pl.multiple_of(block * ROWS, ROWS), ROWS)
    return pl.ds(pl.multiple_of(block * ROWS + half * 128, 128), 128)


def loop(lo, hi, fn):
    def body(i, carry):
        fn(i)
        return carry
    lax.fori_loop(lo, hi, body, 0)


class Gather:
    def __init__(self, full, ss, rs):
        self.full, self.ss, self.rs = full, ss, rs
        self.me, self.core, self.xn, self.yn, self.dg, delta = places()
        me, core, xn, yn, dg = self.me, self.core, self.xn, self.yn, self.dg
        cx, cy, cd = xn + delta, yn + delta, dg + delta
        self.send_rows = [(me, 0), (me, 1), (yn, 1), (me, 1), (me, 0), (xn, 0), (me, None),
                          (xn, 0), (xn, 1), (yn, 1), (yn, 0), (dg, 0), (dg, 1)]
        self.recv_rows = [(xn, 0), (xn, 1), (dg, 1), (yn, 1), (yn, 0), (dg, 0), (core, None),
                          (cx, 0), (cx, 1), (cy, 1), (cy, 0), (cd, 0), (cd, 1)]
        self.peer = [xn] * 3 + [yn] * 3 + [core] * 7

    def copy(self, k, rows):
        ref = self.full.at[rows_at(*rows)]
        return pltpu.make_async_remote_copy(src_ref=ref, dst_ref=ref, send_sem=self.ss.at[k], recv_sem=self.rs.at[k],
                                            device_id={'tp': self.peer[k]}, device_id_type=MESH)

    def barrier(self):
        entry_barrier([self.core, self.xn, self.yn])

    def send(self, k):
        self.copy(k, self.send_rows[k]).start()

    def recv(self, k):
        self.copy(k, self.recv_rows[k]).wait_recv()

    def run(self, compute, pre=None, landed=None):
        def chip(block):
            return pl.multiple_of((block // 2) * CHIP, CHIP)
        for k in (0, 3, 1, 4, 6):
            self.send(k)
        if pre is not None:
            pre()
        self.recv(6)
        compute(0, chip(self.me))
        self.recv(0)
        self.send(5)
        self.send(7)
        self.recv(3)
        self.send(2)
        self.send(9)
        self.recv(1)
        self.send(8)
        self.recv(4)
        self.send(10)
        self.recv(7)
        self.recv(8)
        compute(1, chip(self.xn))
        self.recv(9)
        self.recv(10)
        compute(2, chip(self.yn))
        self.recv(5)
        self.send(11)
        self.recv(2)
        self.send(12)
        if landed is not None:
            landed()
        self.recv(11)
        self.recv(12)
        compute(3, chip(self.dg))
        for k in range(13):
            self.copy(k, self.send_rows[k]).wait_send()


GATHER_SCRATCH = [pltpu.VMEM((SEQ, D), BF), pltpu.SemaphoreType.DMA((13,)), pltpu.SemaphoreType.DMA((13,))]


class Scatter:
    def __init__(self, pb, din, rel, fin, ss, rs):
        self.pb, self.din, self.rel, self.fin, self.ss, self.rs = pb, din, rel, fin, ss, rs
        self.me, self.core, self.xn, self.yn, dg, self.delta = places()
        self.block = [dg, self.xn, self.yn, self.me]

    def barrier(self):
        entry_barrier([self.core, self.xn, self.yn])

    def copy(self, k):
        lo, hi = pl.ds(0, 128), pl.ds(128, 128)
        din, rel, fin, xn, yn = self.din, self.rel, self.fin, self.xn, self.yn
        if not isinstance(k, int) or k < 4:
            src, dst, peer = self.pb.at[k], din.at[k], self.core
        else:
            src, dst, peer = ((din.at[0, lo], rel.at[0], xn), (din.at[1, lo], fin.at[0, lo], xn), (din.at[1, hi], fin.at[0, hi], xn),
                              (din.at[0, hi], rel.at[1], yn), (din.at[2, hi], fin.at[1, hi], yn), (din.at[2, lo], fin.at[1, lo], yn))[k - 4]
        return pltpu.make_async_remote_copy(src_ref=src, dst_ref=dst, send_sem=self.ss.at[k], recv_sem=self.rs.at[k],
                                            device_id={'tp': peer}, device_id_type=MESH)

    def give(self, d, tile, block=None):
        block = self.block[d] + self.delta if block is None else block
        def body(n):
            cols = pl.ds(pl.multiple_of(n * TN, TN), TN)
            self.pb[d, :, cols] = tile(block, n).astype(BF)
        loop(0, D // TN, body)
        self.copy(d).start()

    def keep(self, d, tile):
        self.copy(d).wait_recv()
        def body(n):
            cols = pl.ds(pl.multiple_of(n * TN, TN), TN)
            self.din[d, :, cols] = (tile(self.block[d], n) + self.din[d, :, cols].astype(F32)).astype(BF)
        loop(0, D // TN, body)

    def start(self, *flows):
        for k in flows:
            self.copy(k).start()

    def add_relay(self, d, half, slot):
        def body(n):
            rows = pl.ds(pl.multiple_of(half * 128 + n * 16, 16), 16)
            src = pl.ds(pl.multiple_of(n * 16, 16), 16)
            self.din[d, rows] = (self.din[d, rows].astype(F32) + self.rel[slot, src].astype(F32)).astype(BF)
        loop(0, 8, body)

    def relays(self):
        self.copy(4).wait_recv()
        self.add_relay(2, 0, 0)
        self.start(9)
        self.copy(7).wait_recv()
        self.add_relay(1, 1, 1)
        self.start(6)

    def arrive(self):
        for k in (5, 8, 6, 9):
            self.copy(k).wait_recv()

    def run(self, tile):
        self.give(0, tile)
        self.give(1, tile)
        self.keep(0, tile)
        self.start(4, 7)
        self.give(2, tile)
        self.keep(1, tile)
        self.start(5)
        self.give(3, tile)
        self.keep(2, tile)
        self.start(8)
        self.keep(3, tile)

    def total(self, rows):
        s = self.din[3, rows].astype(F32) + self.fin[0, rows].astype(F32) + self.fin[1, rows].astype(F32)
        return s.astype(BF).astype(F32)

    def finish(self, first=0):
        for k in range(first, 10):
            self.copy(k).wait_send()


SCATTER_REST = [pltpu.VMEM((4, ROWS, D), BF), pltpu.VMEM((2, 128, D), BF), pltpu.VMEM((2, ROWS, D), BF),
                pltpu.SemaphoreType.DMA((10,)), pltpu.SemaphoreType.DMA((10,))]
SCATTER_SCRATCH = [pltpu.VMEM((4, ROWS, D), BF)] + SCATTER_REST
VM = pl.BlockSpec(memory_space=pltpu.VMEM)
HB = pl.BlockSpec(memory_space=pl.ANY)


def call(body, name, cid, ins, outs, scratch, args, flops):
    return pl.pallas_call(
        body,
        name=name,
        out_shape=[jax.ShapeDtypeStruct(s, t) for s, t, _ in outs],
        in_specs=ins,
        out_specs=[m for _, _, m in outs],
        scratch_shapes=scratch,
        compiler_params=pltpu.CompilerParams(collective_id=cid, has_side_effects=True, vmem_limit_bytes=67043328),
        cost_estimate=pl.CostEstimate(flops=flops, bytes_accessed=32 << 20, transcendentals=0),
    )(*args)


def norm_rows(v, gain, bias):
    mean = jnp.mean(v, axis=-1, keepdims=True)
    cent = v - mean
    var = jnp.mean(cent * cent, axis=-1, keepdims=True)
    return cent * lax.rsqrt(var + EPS) * gain + bias


def norm_rows_back(v, gain, ct):
    mean = jnp.mean(v, axis=-1, keepdims=True)
    cent = v - mean
    rstd = lax.rsqrt(jnp.mean(cent * cent, axis=-1, keepdims=True) + EPS)
    xhat = cent * rstd
    gx = ct * gain
    m1 = jnp.mean(gx, axis=-1, keepdims=True)
    m2 = jnp.mean(gx * xhat, axis=-1, keepdims=True)
    return rstd * (gx - m1 - xhat * m2), xhat


RB = 32


def row_blocks(fn):
    loop(0, ROWS // RB, lambda i: fn(pl.ds(pl.multiple_of(i * RB, RB), RB)))


def front_kernel(sl_ref, x_hbm, g1_ref, b1_ref, wq_hbm, bq_ref, gyl_hbm, wo_hbm, bo_ref, g2_ref, b2_ref, wd_hbm,
                 qkv_out, ctx_out, lse_ref, h_out, gy_out, x1_ref, gl_ref, w6_out, ga_out, gbd_ref,
                 full, ss, rs, gyf, ssy, rsy, x, w6, wo, qkv, ctx, bias, biasm, acc, ml, wq, wd, ga, ls, hs, ys, zs, *scratch):
    ag = Gather(full, ss, rs)
    gg = Gather(gyf, ssy, rsy)
    sc = Scatter(*scratch)
    pairs = [(gyl_hbm, gyf.at[rows_at(ag.me)]), (x_hbm, x), (wq_hbm, wq), (wd_hbm, wd), (wo_hbm, wo)]
    loads = [pltpu.make_async_copy(src, dst, ls.at[i]) for i, (src, dst) in enumerate(pairs)]
    for l in loads:
        l.start()
    ag.barrier()
    loads[0].wait()
    for k in (0, 3, 6):
        gg.send(k)
    loads[1].wait()

    def ln(i):
        rows = pl.ds(pl.multiple_of(i * RB, RB), RB)
        dst = pl.ds(pl.multiple_of(ag.me * ROWS + i * RB, RB), RB)
        full[dst] = norm_rows(x[rows].astype(F32), g1_ref[...], b1_ref[...]).astype(BF)
    loop(0, ROWS // RB, ln)
    c1 = (128 ** -0.5) * LOG2E

    def slope(h):
        return sl_ref[2 * ag.me + h] * LOG2E

    def biases():
        ki = lax.broadcasted_iota(jnp.int32, (CHIP, CHIP), 0)
        qi = lax.broadcasted_iota(jnp.int32, (CHIP, CHIP), 1)
        for h in range(2):
            b = ki.astype(F32) * slope(h)
            bias[h] = b
            biasm[h] = jnp.where(ki <= qi, b, MASK_VALUE)
    biases()
    chips = [pl.multiple_of((b // 2) * CHIP, CHIP) for b in (ag.me, ag.xn, ag.yn, ag.dg)]
    gbd_ref[...] = jnp.zeros_like(gbd_ref)

    def act(i):
        rows = pl.ds(chips[i], CHIP)
        def body(n):
            cols = pl.ds(pl.multiple_of(n * 256, 256), 256)
            ga[rows, cols] = dot_nt(gyf[rows], wd[cols]).astype(BF)
        loop(0, 4, body)
        pltpu.make_async_copy(ga.at[rows], ga_out.at[rows], zs.at[i]).start()

    def colsum(n):
        part = pl.ds(pl.multiple_of(n * RB, RB), RB)
        gbd_ref[...] += jnp.sum(gyf[part].astype(F32), axis=0, keepdims=True)

    def weights():
        for l in loads[2:]:
            l.wait()
        def body(i):
            part = pl.ds(pl.multiple_of(i * CHIP, CHIP), CHIP)
            for t in range(3):
                for h in range(2):
                    w6[2 * t + h, part] = wq[part, t, h]
        loop(0, 4, body)
        pltpu.make_async_copy(w6, w6_out, ls.at[2]).start()
        gg.recv(6)
        act(0)

    def compute(idx, r0):
        rows = pl.ds(r0, CHIP)
        pltpu.make_async_copy(full.at[rows], h_out.at[rows], hs.at[idx]).start()
        def body(t):
            cols = pl.ds(pl.multiple_of(t * 256, 256), 256)
            w = jnp.concatenate([w6[2 * t], w6[2 * t + 1]], axis=1)
            qkv[rows, cols] = (dot(full[rows], w) + bq_ref[:, cols]).astype(BF)
        loop(0, 3, body)

    def start_gy():
        gg.send(1)
        gg.send(4)
        gg.recv(0)
        gg.send(5)
        gg.send(7)
        gg.recv(3)
        gg.send(2)
        gg.send(9)
    ag.run(compute, pre=weights, landed=start_gy)
    stores = [pltpu.make_async_copy(qkv, qkv_out, ls.at[0]), pltpu.make_async_copy(ctx, ctx_out, ls.at[1]),
              pltpu.make_async_copy(w6, w6_out, ls.at[2])]
    stores[0].start()

    def tile(block, n):
        cols = pl.ds(pl.multiple_of(n * TN, TN), TN)
        return dot(ctx[rows_at(block)], wo[:, cols])

    xb = lax.rem(ag.me // 2, 2)
    yb = ag.me // 4

    def attend(p):
        nx = xb + (1 - p // 2) * (1 - 2 * xb)
        ny = yb + (1 - lax.rem(p, 2)) * (1 - 2 * yb)
        i = 2 * ny + nx
        qrows = pl.ds(pl.multiple_of(i * CHIP, CHIP), CHIP)

        def one(h):
            lanes = [pl.ds(pl.multiple_of((2 * t + h) * 128, 128), 128) for t in range(3)]
            sl = slope(h)
            q = qkv[qrows, lanes[0]]
            ml[0:1] = jnp.full((1, CHIP), MASK_VALUE, F32)
            ml[1:2] = jnp.zeros((1, CHIP), F32)
            acc[...] = jnp.zeros_like(acc)
            def step(j, bias_ref):
                krows = pl.ds(pl.multiple_of(j * CHIP, CHIP), CHIP)
                s = dot_nt(qkv[krows, lanes[1]], q) * c1 + bias_ref[h]
                cj = sl * (j * CHIP).astype(F32)
                m = ml[0:1]
                mn = jnp.maximum(m, jnp.max(s, axis=0, keepdims=True) + cj)
                pr = jnp.exp2(s - (mn - cj))
                alpha = jnp.exp2(m - mn)
                ml[1:2] = ml[1:2] * alpha + jnp.sum(pr, axis=0, keepdims=True)
                ml[0:1] = mn
                acc[...] = acc[...] * alpha + dot_tn(qkv[krows, lanes[2]], pr.astype(BF))
            loop(0, i, lambda j: step(j, bias))
            step(i, biasm)
            ctx[qrows, lanes[0]] = jnp.transpose(acc[...] / ml[1:2]).astype(BF)
            lse_ref[h, :, qrows] = ml[0:1] + jnp.log(ml[1:2]) * LOG2E
        loop(0, 2, one)
        sc.give(p, tile, 2 * i + 1 - lax.rem(ag.me, 2))
    loop(0, 4, attend)
    stores[1].start()

    sc.keep(0, tile)
    sc.start(4, 7)
    sc.keep(1, tile)
    sc.start(5)
    sc.keep(2, tile)
    sc.start(8)
    sc.keep(3, tile)
    gg.recv(1)
    gg.send(8)
    gg.recv(4)
    gg.send(10)

    def keep_gy(i):
        rows = pl.ds(chips[i], CHIP)
        return pltpu.make_async_copy(gyf.at[rows], gy_out.at[rows], ys.at[i])
    keep_gy(0).start()
    gg.recv(7)
    gg.recv(8)
    keep_gy(1).start()
    act(1)
    gg.recv(5)
    gg.send(11)
    gg.recv(2)
    gg.send(12)
    gg.recv(9)
    gg.recv(10)
    keep_gy(2).start()
    act(2)
    gg.recv(11)
    gg.recv(12)
    keep_gy(3).start()
    sc.relays()
    act(3)
    loop(0, SEQ // RB, colsum)
    sc.arrive()

    def fin(rows):
        x1 = x[rows].astype(F32) + sc.total(rows) + bo_ref[...]
        x1_ref[rows] = x1
        gl_ref[rows] = norm_rows(x1, g2_ref[...], b2_ref[...]).astype(BF)
    row_blocks(fin)
    sc.finish()
    for k in range(13):
        gg.copy(k, gg.send_rows[k]).wait_send()
    for s in stores:
        s.wait()
    for i in range(4):
        rows = pl.ds(i * CHIP, CHIP)
        pltpu.make_async_copy(full.at[rows], h_out.at[rows], hs.at[i]).wait()
        pltpu.make_async_copy(ga.at[rows], ga_out.at[rows], zs.at[i]).wait()
        keep_gy(i).wait()


def mlp_kernel(g_hbm, gy_hbm, wu_hbm, bu_ref, ga_hbm, x1_hbm, g2_ref,
               r_out, gm_ref, gmb_ref, vec_ref, gwu_out, gwd_out, gbu_ref,
               full, ss, rs, gy, wu, x1, gp, r, gw, ls, ys, *scratch):
    ag = Gather(full, ss, rs)
    sc = Scatter(*scratch)
    own = pltpu.make_async_copy(g_hbm, full.at[rows_at(ag.me)], ls.at[0])
    own.start()
    chips = [pl.multiple_of((b // 2) * CHIP, CHIP) for b in (ag.me, ag.xn, ag.yn, ag.dg)]
    load_wu = pltpu.make_async_copy(wu_hbm, wu, ls.at[2])
    load_wu.start()
    load_ga = pltpu.make_async_copy(ga_hbm, gp, ls.at[1])
    load_ga.start()
    load_gy = pltpu.make_async_copy(gy_hbm, gy, ys.at[0])
    load_x1 = pltpu.make_async_copy(x1_hbm, x1, ls.at[3])
    load_x1.start()
    own.wait()
    ag.barrier()
    for k in (0, 3, 1, 4, 6):
        ag.send(k)
    gbu_ref[...] = jnp.zeros_like(gbu_ref)
    vec_ref[...] = jnp.zeros_like(vec_ref)
    load_gy.start()

    k0 = math.sqrt(2.0 / math.pi)
    k1 = 0.044715

    def up(i):
        rows = pl.ds(chips[i], CHIP)
        def body(n):
            cols = pl.ds(pl.multiple_of(n * 256, 256), 256)
            z = dot(full[rows], wu[:, cols]) + bu_ref[:, cols]
            z2 = z * z
            t = jnp.tanh(k0 * (z + k1 * (z2 * z)))
            half = 0.5 * (1.0 + t)
            r[rows, cols] = (z * half).astype(BF)
            dz = half + (0.5 * z) * (1.0 - t * t) * (k0 * (1.0 + 3.0 * k1 * z2))
            gpre = gp[rows, cols].astype(F32) * dz
            gbu_ref[:, cols] += jnp.sum(gpre, axis=0, keepdims=True)
            gp[rows, cols] = gpre.astype(BF)
        loop(0, 4, body)
        pltpu.make_async_copy(r.at[rows], r_out.at[rows], ys.at[i]).start()

    def tile(block, n):
        cols = pl.ds(pl.multiple_of(n * TN, TN), TN)
        return dot_nt(gp[rows_at(block)], wu[cols])

    load_wu.wait()
    load_ga.wait()
    load_gy.wait()
    ag.recv(6)
    up(0)
    ag.recv(0)
    ag.send(5)
    ag.send(7)
    ag.recv(3)
    ag.send(2)
    ag.send(9)
    ag.recv(1)
    ag.send(8)
    ag.recv(4)
    ag.send(10)
    ag.recv(7)
    ag.recv(8)
    up(1)
    sc.give(1, tile)
    ag.recv(9)
    ag.recv(10)
    up(2)
    sc.give(2, tile)
    ag.recv(5)
    ag.send(11)
    ag.recv(2)
    ag.send(12)
    sc.keep(1, tile)
    sc.start(5)
    sc.keep(2, tile)
    sc.start(8)
    ag.recv(11)
    ag.recv(12)
    up(3)
    sc.give(0, tile)
    sc.give(3, tile)
    sc.keep(0, tile)
    sc.start(4, 7)
    sc.keep(3, tile)

    def gwu_step(i):
        cols = pl.ds(pl.multiple_of(i * 256, 256), 256)
        gw[:, pl.ds(0, 1024)] = dot_tn(full[:, cols], gp[...]).astype(BF)
        c = pltpu.make_async_copy(gw.at[:, pl.ds(0, 1024)], gwu_out.at[cols], ls.at[4])
        c.start()
        c.wait()

    def gwd_step(i):
        cols = pl.ds(pl.multiple_of(i * 256, 256), 256)
        gw[...] = dot_tn(r[:, cols], gy[...]).astype(BF)
        c = pltpu.make_async_copy(gw, gwd_out.at[cols], ls.at[4])
        c.start()
        c.wait()

    loop(0, 6, gwu_step)
    sc.relays()
    loop(6, 8, gwu_step)
    loop(0, 4, gwd_step)
    load_x1.wait()
    sc.arrive()

    def fin(rows):
        ct = sc.total(rows)
        dx, xhat = norm_rows_back(x1[rows], g2_ref[...], ct)
        mine = pl.ds(pl.multiple_of(ag.me * ROWS + rows.start, RB), RB)
        gm = gy[mine].astype(F32) + dx
        gm_ref[rows] = gm
        gmb_ref[rows] = gm.astype(BF)
        vec_ref[0:1] += jnp.sum(ct * xhat, axis=0, keepdims=True)
        vec_ref[1:2] += jnp.sum(ct, axis=0, keepdims=True)
        vec_ref[2:3] += jnp.sum(gm, axis=0, keepdims=True)
    row_blocks(fin)
    for k in range(13):
        ag.copy(k, ag.send_rows[k]).wait_send()
    sc.finish()
    for i in range(4):
        rows = pl.ds(chips[i], CHIP)
        pltpu.make_async_copy(r.at[rows], r_out.at[rows], ys.at[i]).wait()


def tail_kernel(sl_ref, gm_hbm, wo_hbm, r_hbm, wd_hbm, qkv_hbm, ctx_hbm, lse_ref, w6_hbm, x_hbm, gmf_hbm, x1_hbm, bd_ref, g1_ref,
                h_hbm, vec2_ref, y_ref, gx_ref, vec_out, gwq_out, gwo_out, gb_ref,
                full, ss, rs, wo, r, wd, qkv, ctx, w6, x1, gc, gq, gwq, gwo, bias, biasm, delta, dqt, dk, dv, vec, bufv,
                ls, vs, vr, pb, din1, rel1, fin1, ss1, rs1, din2, rel2, fin2, ss2, rs2):
    ag = Gather(full, ss, rs)
    s1 = Scatter(pb, din1, rel1, fin1, ss1, rs1)
    s2 = Scatter(pb, din2, rel2, fin2, ss2, rs2)
    pairs = [(gm_hbm, full.at[rows_at(ag.me)]), (wd_hbm, wd), (r_hbm, r), (wo_hbm, wo), (qkv_hbm, qkv), (ctx_hbm, ctx), (w6_hbm, w6),
             (x1_hbm, x1)]
    loads = [pltpu.make_async_copy(src, dst, ls.at[i]) for i, (src, dst) in enumerate(pairs)]
    for l in loads:
        l.start()
    loads[0].wait()
    peers = [lax.rem(ag.me + k, 8) for k in range(1, 8)]
    entry_barrier(peers)
    for k in (0, 3, 1, 4, 6):
        ag.send(k)
    scale = 128 ** -0.5
    c1 = scale * LOG2E
    vec[...] = vec2_ref[...]
    gb_ref[...] = jnp.zeros_like(gb_ref)

    def mtile(block, n):
        cols = pl.ds(pl.multiple_of(n * TN, TN), TN)
        return dot(r[rows_at(block)], wd[:, cols])

    def gcs(block):
        rows = pl.ds(pl.multiple_of((block // 2) * CHIP, CHIP), CHIP)
        gc[rows] = dot_nt(full[rows], wo[...]).astype(BF)

    loads[1].wait()
    loads[2].wait()
    for d in range(4):
        s1.give(d, mtile)
    s1.keep(0, mtile)
    loads[3].wait()
    ag.recv(6)
    gcs(ag.me)
    ag.recv(0)
    ag.send(5)
    ag.send(7)
    ag.recv(3)
    ag.send(2)
    ag.send(9)
    for d in range(1, 4):
        s1.keep(d, mtile)
    load_h = [pltpu.make_async_copy(h_hbm.at[:, pl.ds(i * 1024, 1024)], r, ls.at[10 + i]) for i in range(2)]
    load_h[0].start()
    for l in loads[4:]:
        l.wait()

    def rowsum(i):
        rows = pl.ds(pl.multiple_of(i * CHIP, CHIP), CHIP)
        for h in range(2):
            lanes = pl.ds(h * 128, 128)
            prod = gc[rows, lanes].astype(F32) * ctx[rows, lanes].astype(F32)
            delta[h:h + 1, rows] = jnp.sum(jnp.transpose(prod), axis=0, keepdims=True)

    ag.recv(1)
    ag.send(8)
    ag.recv(4)
    ag.send(10)
    ag.recv(7)
    ag.recv(8)
    gcs(ag.xn)
    ag.recv(9)
    ag.recv(10)
    gcs(ag.yn)
    ag.recv(5)
    ag.send(11)
    ag.recv(2)
    ag.send(12)
    s1.start(4, 7, 5, 8)
    ag.recv(11)
    ag.recv(12)
    gcs(ag.dg)
    x = wo
    load_x = pltpu.make_async_copy(x_hbm, x, ls.at[8])
    load_x.start()
    loop(0, SEQ // CHIP, rowsum)

    def put(h, t, rows, val):
        val = val.astype(BF)
        gq[rows, (2 * t + h) * 128:(2 * t + h + 1) * 128] = val
        gb_ref[t, h:h + 1] += jnp.sum(val.astype(F32), axis=0, keepdims=True)

    def head(h):
        sl = sl_ref[2 * ag.me + h] * LOG2E
        ki = lax.broadcasted_iota(jnp.int32, (CHIP, CHIP), 0)
        qi = lax.broadcasted_iota(jnp.int32, (CHIP, CHIP), 1)
        b = ki.astype(F32) * sl
        bias[...] = b
        biasm[...] = jnp.where(ki <= qi, b, MASK_VALUE)
        dqt[...] = jnp.zeros_like(dqt)
        lq, lk, lv, lo = (pl.ds((2 * t + h) * 128, 128) for t in (0, 1, 2, 0))

        def kblock(j):
            krows = pl.ds(pl.multiple_of(j * CHIP, CHIP), CHIP)
            k = qkv[krows, lk]
            v = qkv[krows, lv]
            dk[...] = jnp.zeros_like(dk)
            dv[...] = jnp.zeros_like(dv)
            cj = sl * (j * CHIP).astype(F32)
            def step(i, bias_ref):
                qrows = pl.ds(pl.multiple_of(i * CHIP, CHIP), CHIP)
                q = qkv[qrows, lq]
                do = gc[qrows, lo]
                p = jnp.exp2(dot_nt(k, q) * c1 + bias_ref[...] - (lse_ref[h, :, qrows] - cj))
                dv[...] += dot(p.astype(BF), do)
                ds = (p * (dot_nt(v, do) - delta[h:h + 1, qrows])).astype(BF)
                dk[...] += dot(ds, q)
                dqt[:, qrows] += dot_tn(k, ds)
            step(j, biasm)
            loop(j + 1, SEQ // CHIP, lambda i: step(i, bias))
            put(h, 1, krows, dk[...] * scale)
            put(h, 2, krows, dv[...])
        loop(0, SEQ // CHIP, kblock)

        def qout(i):
            rows = pl.ds(pl.multiple_of(i * CHIP, CHIP), CHIP)
            put(h, 0, rows, jnp.transpose(dqt[:, rows]) * scale)
        loop(0, SEQ // CHIP, qout)

    head(0)
    s1.relays()
    head(1)

    def htile(block, n):
        rows = rows_at(block)
        cols = pl.ds(pl.multiple_of(n * TN, TN), TN)
        out = None
        for t in range(3):
            w = jnp.concatenate([w6[2 * t, cols], w6[2 * t + 1, cols]], axis=1)
            part = dot_nt(gq[rows, t * 256:(t + 1) * 256], w)
            out = part if out is None else out + part
        return out

    for k in range(4):
        s1.copy(k).wait_send()
    s2.run(htile)

    stores = [pltpu.make_async_copy(gwq, gwq_out.at[pl.ds(i * 1024, 1024)], ls.at[12]) for i in range(2)]
    stores.append(pltpu.make_async_copy(gwo, gwo_out, ls.at[13]))

    def wq():
        def body(i):
            src = pl.ds(pl.multiple_of(i * 256, 256), 256)
            val = dot_tn(r[:, src], gq[...])
            for t in range(3):
                pair = [val[:, (2 * t + h) * 128:(2 * t + h + 1) * 128] for h in range(2)]
                gwq[src, t] = jnp.stack(pair, axis=1).astype(BF)
        return body

    load_h[0].wait()
    loop(0, 4, wq())
    load_h[1].start()
    stores[0].start()
    s2.relays()
    s1.arrive()

    def yrow(rows):
        y_ref[rows] = (x1[rows] + s1.total(rows) + bd_ref[...]).astype(BF)
    row_blocks(yrow)
    gm = x1
    load_gm = pltpu.make_async_copy(gmf_hbm, gm, ls.at[9])
    load_gm.start()

    def wout(n):
        cols = pl.ds(pl.multiple_of(n * TN, TN), TN)
        gwo[:, cols] = dot_tn(ctx[...], full[:, cols]).astype(BF)
    loop(0, D // TN, wout)
    stores[2].start()
    load_h[1].wait()
    stores[0].wait()
    loop(0, 4, wq())
    stores[1].start()
    load_x.wait()
    load_gm.wait()
    s2.arrive()

    def fin(rows):
        ct = s2.total(rows)
        dx, xhat = norm_rows_back(x[rows].astype(F32), g1_ref[...], ct)
        gx_ref[rows] = (gm[rows] + dx).astype(BF)
        vec[3:4] += jnp.sum(ct * xhat, axis=0, keepdims=True)
        vec[4:5] += jnp.sum(ct, axis=0, keepdims=True)
    row_blocks(fin)
    s1.finish(4)
    s2.finish()
    copies = [pltpu.make_async_remote_copy(src_ref=vec, dst_ref=bufv.at[ag.me], send_sem=vs.at[k], recv_sem=vr.at[k],
                                           device_id={'tp': peers[k]}, device_id_type=MESH) for k in range(7)]
    for c in copies:
        c.start()
    bufv[ag.me] = vec[...]
    for k in range(13):
        ag.copy(k, ag.send_rows[k]).wait_send()
    for s in stores[1:]:
        s.wait()
    for c in copies:
        c.wait()
    total = bufv[0]
    for i in range(1, 8):
        total = total + bufv[i]
    vec_out[...] = total


def solution(mesh):
    def local_step(x, ln1_gamma, ln1_beta, w_qkv, b_qkv, w_out, b_out, ln2_gamma, ln2_beta, w_up, b_up, w_down, b_down, grad_y):
        slopes = alibi_slopes(16)
        row = lambda v: v.reshape(1, -1)
        x2, gy2 = x[0], grad_y[0]
        bq = b_qkv.transpose(1, 0, 2).reshape(1, 768)

        qkv, ctx, lse, h_full, gy_full, x1, g_loc, w6, ga, gbd = call(
            front_kernel, 'front', 0, [pl.BlockSpec(memory_space=pltpu.SMEM), HB, VM, VM, HB, VM, HB, HB, VM, VM, VM, HB],
            [((SEQ, 768), BF, HB), ((SEQ, 256), BF, HB), ((2, 1, SEQ), F32, VM), ((SEQ, D), BF, HB), ((SEQ, D), BF, HB),
             ((ROWS, D), F32, VM), ((ROWS, D), BF, VM), ((6, D, 128), BF, HB), ((SEQ, 1024), BF, HB), ((1, D), F32, VM)],
            GATHER_SCRATCH * 2 + [pltpu.VMEM((ROWS, D), BF), pltpu.VMEM((6, D, 128), BF), pltpu.VMEM((256, D), BF),
                                  pltpu.VMEM((SEQ, 768), BF), pltpu.VMEM((SEQ, 256), BF), pltpu.VMEM((2, CHIP, CHIP), F32),
                                  pltpu.VMEM((2, CHIP, CHIP), F32), pltpu.VMEM((128, CHIP), F32), pltpu.VMEM((8, CHIP), F32),
                                  pltpu.VMEM((D, 3, 2, 128), BF), pltpu.VMEM((1024, D), BF), pltpu.VMEM((SEQ, 1024), BF),
                                  pltpu.SemaphoreType.DMA((5,))] + [pltpu.SemaphoreType.DMA((4,))] * 3
            + SCATTER_SCRATCH,
            (slopes, x2, row(ln1_gamma), row(ln1_beta), w_qkv.transpose(0, 2, 1, 3), bq, gy2, w_out, row(b_out), row(ln2_gamma),
             row(ln2_beta), w_down), 20 << 30)
        r, gm, gm_bf, vec2, g_wu, g_wd, gbu = call(
            mlp_kernel, 'mlp', 2, [HB, HB, HB, VM, HB, HB, VM],
            [((SEQ, 1024), BF, HB), ((ROWS, D), F32, VM), ((ROWS, D), BF, VM), ((8, D), F32, VM), ((D, 1024), BF, HB),
             ((1024, D), BF, HB), ((1, 1024), F32, VM)],
            GATHER_SCRATCH + [pltpu.VMEM((SEQ, D), BF), pltpu.VMEM((D, 1024), BF), pltpu.VMEM((ROWS, D), F32),
                              pltpu.VMEM((SEQ, 1024), BF), pltpu.VMEM((SEQ, 1024), BF), pltpu.VMEM((256, D), BF),
                              pltpu.SemaphoreType.DMA((5,)), pltpu.SemaphoreType.DMA((4,))] + SCATTER_SCRATCH,
            (g_loc, gy_full, w_up, row(b_up), ga, x1, row(ln2_gamma)), 36 << 30)
        y, g_x, vec, g_wq, g_wo, g_bq = call(
            tail_kernel, 'tail', 3, [pl.BlockSpec(memory_space=pltpu.SMEM)] + [HB] * 6 + [VM] + [HB] * 4 + [VM] * 2 + [HB, VM],
            [((ROWS, D), BF, VM), ((ROWS, D), BF, VM), ((8, D), F32, VM), ((D, 3, 2, 128), BF, HB), ((256, D), BF, HB), ((3, 2, 128), F32, VM)],
            GATHER_SCRATCH + [pltpu.VMEM((256, D), BF), pltpu.VMEM((SEQ, 1024), BF), pltpu.VMEM((1024, D), BF), pltpu.VMEM((SEQ, 768), BF),
                              pltpu.VMEM((SEQ, 256), BF), pltpu.VMEM((6, D, 128), BF), pltpu.VMEM((ROWS, D), F32),
                              pltpu.VMEM((SEQ, 256), BF), pltpu.VMEM((SEQ, 768), BF), pltpu.VMEM((1024, 3, 2, 128), BF),
                              pltpu.VMEM((256, D), BF), pltpu.VMEM((CHIP, CHIP), F32), pltpu.VMEM((CHIP, CHIP), F32),
                              pltpu.VMEM((2, SEQ), F32), pltpu.VMEM((128, SEQ), F32), pltpu.VMEM((CHIP, 128), F32),
                              pltpu.VMEM((CHIP, 128), F32), pltpu.VMEM((8, D), F32), pltpu.VMEM((8, 8, D), F32),
                              pltpu.SemaphoreType.DMA((14,)), pltpu.SemaphoreType.DMA((7,)), pltpu.SemaphoreType.DMA((7,))]
            + SCATTER_SCRATCH + SCATTER_REST,
            (slopes, gm_bf, w_out, r, w_down, qkv, ctx, lse, w6, x2, gm, x1, row(b_down), row(ln1_gamma), h_full, vec2), 55 << 30)
        g_wq, g_bq = g_wq.transpose(0, 2, 1, 3), g_bq.transpose(1, 0, 2)
        return (y[None], g_x[None], vec[3], vec[4], g_wq, g_bq, g_wo, vec[2], vec[0], vec[1], g_wu, gbu[0], g_wd, gbd[0])

    row_spec = P('dp', 'tp', None)
    in_specs = (row_spec, P(), P(), P(None, 'tp', None, None), P('tp', None, None), P('tp', None), P(), P(), P(),
                P(None, 'tp'), P('tp'), P('tp', None), P(), row_spec)
    out_specs = (row_spec, row_spec, P('dp'), P('dp'), P('dp', 'tp', None, None), P(('dp', 'tp'), None, None),
                 P(('dp', 'tp'), None), P('dp'), P('dp'), P('dp'), P('dp', 'tp'), P(('dp', 'tp')), P(('dp', 'tp'), None), P('dp'))
    return jax.shard_map(local_step, mesh=mesh, in_specs=in_specs, out_specs=out_specs, check_vma=False)
```

```python
import functools
import math
import jax
import jax.numpy as jnp
from jax import lax
from jax.experimental import pallas as pl
from jax.experimental.pallas import tpu as pltpu
from jax.sharding import PartitionSpec as P

EPS = 1e-5
MASK_VALUE = -1e30
LOG2E = math.log2(math.e)
MESH = pl.DeviceIdType.MESH
BF = jnp.bfloat16
F32 = jnp.float32
ROWS = 256
CHIP = 512
SEQ = 2048
D = 2048
TN = 512


def alibi_slopes(n_heads):
    closest = 2 ** int(math.floor(math.log2(n_heads)))
    base_ratio = 2.0 ** (-8.0 / closest)
    extra_ratio = 2.0 ** (-4.0 / closest)
    remaining = min(closest, n_heads - closest)
    slopes = [base_ratio ** (i + 1) for i in range(closest)]
    slopes = slopes + [extra_ratio ** (2 * i + 1) for i in range(remaining)]
    return jnp.array(slopes, dtype=jnp.float32)


def dot(a, b):
    return lax.dot_general(a, b, (((1,), (0,)), ((), ())), preferred_element_type=F32)


def dot_nt(a, b):
    return lax.dot_general(a, b, (((1,), (1,)), ((), ())), preferred_element_type=F32)


def dot_tn(a, b):
    return lax.dot_general(a, b, (((0,), (0,)), ((), ())), preferred_element_type=F32)


def places():
    me = lax.axis_index('tp')
    c = lax.rem(me, 2)
    delta = 1 - 2 * c
    xn = me + 2 - 4 * lax.rem(me // 2, 2)
    dy = 4 - 8 * (me // 4)
    return me, me + delta, xn, me + dy, xn + dy, delta


def entry_barrier(peers):
    sem = pltpu.get_barrier_semaphore()
    for p in peers:
        pl.semaphore_signal(sem, inc=1, device_id={'tp': p}, device_id_type=MESH)
    pl.semaphore_wait(sem, len(peers))


def rows_at(block, half=None):
    if half is None:
        return pl.ds(pl.multiple_of(block * ROWS, ROWS), ROWS)
    return pl.ds(pl.multiple_of(block * ROWS + half * 128, 128), 128)


def loop(lo, hi, fn):
    def body(i, carry):
        fn(i)
        return carry
    lax.fori_loop(lo, hi, body, 0)


class Gather:
    def __init__(self, full, ss, rs):
        self.full, self.ss, self.rs = full, ss, rs
        self.me, self.core, self.xn, self.yn, self.dg, delta = places()
        me, core, xn, yn, dg = self.me, self.core, self.xn, self.yn, self.dg
        cx, cy, cd = xn + delta, yn + delta, dg + delta
        self.send_rows = [(me, 0), (me, 1), (yn, 1), (me, 1), (me, 0), (xn, 0), (me, None),
                          (xn, 0), (xn, 1), (yn, 1), (yn, 0), (dg, 0), (dg, 1)]
        self.recv_rows = [(xn, 0), (xn, 1), (dg, 1), (yn, 1), (yn, 0), (dg, 0), (core, None),
                          (cx, 0), (cx, 1), (cy, 1), (cy, 0), (cd, 0), (cd, 1)]
        self.peer = [xn] * 3 + [yn] * 3 + [core] * 7

    def copy(self, k, rows):
        ref = self.full.at[rows_at(*rows)]
        return pltpu.make_async_remote_copy(src_ref=ref, dst_ref=ref, send_sem=self.ss.at[k], recv_sem=self.rs.at[k],
                                            device_id={'tp': self.peer[k]}, device_id_type=MESH)

    def barrier(self):
        entry_barrier([self.core, self.xn, self.yn])

    def send(self, k):
        self.copy(k, self.send_rows[k]).start()

    def recv(self, k):
        self.copy(k, self.recv_rows[k]).wait_recv()

    def run(self, compute, pre=None, landed=None):
        def chip(block):
            return pl.multiple_of((block // 2) * CHIP, CHIP)
        for k in (0, 3, 1, 4, 6):
            self.send(k)
        if pre is not None:
            pre()
        self.recv(6)
        compute(0, chip(self.me))
        self.recv(0)
        self.send(5)
        self.send(7)
        self.recv(3)
        self.send(2)
        self.send(9)
        self.recv(1)
        self.send(8)
        self.recv(4)
        self.send(10)
        self.recv(7)
        self.recv(8)
        compute(1, chip(self.xn))
        self.recv(9)
        self.recv(10)
        compute(2, chip(self.yn))
        self.recv(5)
        self.send(11)
        self.recv(2)
        self.send(12)
        if landed is not None:
            landed()
        self.recv(11)
        self.recv(12)
        compute(3, chip(self.dg))
        for k in range(13):
            self.copy(k, self.send_rows[k]).wait_send()


GATHER_SCRATCH = [pltpu.VMEM((SEQ, D), BF), pltpu.SemaphoreType.DMA((13,)), pltpu.SemaphoreType.DMA((13,))]


class Scatter:
    def __init__(self, pb, din, rel, fin, ss, rs):
        self.pb, self.din, self.rel, self.fin, self.ss, self.rs = pb, din, rel, fin, ss, rs
        self.me, self.core, self.xn, self.yn, dg, self.delta = places()
        self.block = [dg, self.xn, self.yn, self.me]

    def barrier(self):
        entry_barrier([self.core, self.xn, self.yn])

    def copy(self, k):
        lo, hi = pl.ds(0, 128), pl.ds(128, 128)
        din, rel, fin, xn, yn = self.din, self.rel, self.fin, self.xn, self.yn
        if not isinstance(k, int) or k < 4:
            src, dst, peer = self.pb.at[k], din.at[k], self.core
        else:
            src, dst, peer = ((din.at[0, lo], rel.at[0], xn), (din.at[1, lo], fin.at[0, lo], xn), (din.at[1, hi], fin.at[0, hi], xn),
                              (din.at[0, hi], rel.at[1], yn), (din.at[2, hi], fin.at[1, hi], yn), (din.at[2, lo], fin.at[1, lo], yn))[k - 4]
        return pltpu.make_async_remote_copy(src_ref=src, dst_ref=dst, send_sem=self.ss.at[k], recv_sem=self.rs.at[k],
                                            device_id={'tp': peer}, device_id_type=MESH)

    def give(self, d, tile, block=None):
        block = self.block[d] + self.delta if block is None else block
        def body(n):
            cols = pl.ds(pl.multiple_of(n * TN, TN), TN)
            self.pb[d, :, cols] = tile(block, n).astype(BF)
        loop(0, D // TN, body)
        self.copy(d).start()

    def keep(self, d, tile):
        self.copy(d).wait_recv()
        def body(n):
            cols = pl.ds(pl.multiple_of(n * TN, TN), TN)
            self.din[d, :, cols] = (tile(self.block[d], n) + self.din[d, :, cols].astype(F32)).astype(BF)
        loop(0, D // TN, body)

    def start(self, *flows):
        for k in flows:
            self.copy(k).start()

    def add_relay(self, d, half, slot):
        def body(n):
            rows = pl.ds(pl.multiple_of(half * 128 + n * 16, 16), 16)
            src = pl.ds(pl.multiple_of(n * 16, 16), 16)
            self.din[d, rows] = (self.din[d, rows].astype(F32) + self.rel[slot, src].astype(F32)).astype(BF)
        loop(0, 8, body)

    def relays(self):
        self.copy(4).wait_recv()
        self.add_relay(2, 0, 0)
        self.start(9)
        self.copy(7).wait_recv()
        self.add_relay(1, 1, 1)
        self.start(6)

    def arrive(self):
        for k in (5, 8, 6, 9):
            self.copy(k).wait_recv()

    def run(self, tile):
        self.give(0, tile)
        self.give(1, tile)
        self.keep(0, tile)
        self.start(4, 7)
        self.give(2, tile)
        self.keep(1, tile)
        self.start(5)
        self.give(3, tile)
        self.keep(2, tile)
        self.start(8)
        self.keep(3, tile)

    def total(self, rows):
        s = self.din[3, rows].astype(F32) + self.fin[0, rows].astype(F32) + self.fin[1, rows].astype(F32)
        return s.astype(BF).astype(F32)

    def finish(self, first=0):
        for k in range(first, 10):
            self.copy(k).wait_send()


SCATTER_REST = [pltpu.VMEM((4, ROWS, D), BF), pltpu.VMEM((2, 128, D), BF), pltpu.VMEM((2, ROWS, D), BF),
                pltpu.SemaphoreType.DMA((10,)), pltpu.SemaphoreType.DMA((10,))]
SCATTER_SCRATCH = [pltpu.VMEM((4, ROWS, D), BF)] + SCATTER_REST
VM = pl.BlockSpec(memory_space=pltpu.VMEM)
HB = pl.BlockSpec(memory_space=pl.ANY)


def call(body, name, cid, ins, outs, scratch, args, flops):
    return pl.pallas_call(
        body,
        name=name,
        out_shape=[jax.ShapeDtypeStruct(s, t) for s, t, _ in outs],
        in_specs=ins,
        out_specs=[m for _, _, m in outs],
        scratch_shapes=scratch,
        compiler_params=pltpu.CompilerParams(collective_id=cid, has_side_effects=True, vmem_limit_bytes=67043328),
        cost_estimate=pl.CostEstimate(flops=flops, bytes_accessed=32 << 20, transcendentals=0),
    )(*args)


def norm_rows(v, gain, bias):
    mean = jnp.mean(v, axis=-1, keepdims=True)
    cent = v - mean
    var = jnp.mean(cent * cent, axis=-1, keepdims=True)
    return cent * lax.rsqrt(var + EPS) * gain + bias


def norm_rows_back(v, gain, ct):
    mean = jnp.mean(v, axis=-1, keepdims=True)
    cent = v - mean
    rstd = lax.rsqrt(jnp.mean(cent * cent, axis=-1, keepdims=True) + EPS)
    xhat = cent * rstd
    gx = ct * gain
    m1 = jnp.mean(gx, axis=-1, keepdims=True)
    m2 = jnp.mean(gx * xhat, axis=-1, keepdims=True)
    return rstd * (gx - m1 - xhat * m2), xhat


RB = 32


def row_blocks(fn):
    loop(0, ROWS // RB, lambda i: fn(pl.ds(pl.multiple_of(i * RB, RB), RB)))


def front_kernel(sl_ref, x_hbm, g1_ref, b1_ref, wq_hbm, bq_ref, gyl_hbm, wo_hbm, bo_ref, g2_ref, b2_ref, wd_hbm,
                 qkv_out, ctx_out, lse_ref, h_out, gy_out, x1_ref, gl_ref, w6_out, ga_out, gbd_ref,
                 full, ss, rs, gyf, ssy, rsy, x, w6, wo, qkv, ctx, bias, biasm, acc, ml, wq, wd, ga, ls, hs, ys, zs, *scratch):
    ag = Gather(full, ss, rs)
    gg = Gather(gyf, ssy, rsy)
    sc = Scatter(*scratch)
    pairs = [(gyl_hbm, gyf.at[rows_at(ag.me)]), (x_hbm, x), (wq_hbm, wq), (wd_hbm, wd), (wo_hbm, wo)]
    loads = [pltpu.make_async_copy(src, dst, ls.at[i]) for i, (src, dst) in enumerate(pairs)]
    for l in loads[:2]:
        l.start()
    ag.barrier()
    loads[0].wait()
    for k in (0, 3, 6):
        gg.send(k)
    loads[1].wait()
    for l in loads[2:]:
        l.start()

    def ln(i):
        rows = pl.ds(pl.multiple_of(i * RB, RB), RB)
        dst = pl.ds(pl.multiple_of(ag.me * ROWS + i * RB, RB), RB)
        full[dst] = norm_rows(x[rows].astype(F32), g1_ref[...], b1_ref[...]).astype(BF)
    loop(0, ROWS // RB, ln)
    c1 = (128 ** -0.5) * LOG2E

    def slope(h):
        return sl_ref[2 * ag.me + h] * LOG2E

    def biases():
        ki = lax.broadcasted_iota(jnp.int32, (CHIP, CHIP), 0)
        qi = lax.broadcasted_iota(jnp.int32, (CHIP, CHIP), 1)
        for h in range(2):
            b = ki.astype(F32) * slope(h)
            bias[h] = b
            biasm[h] = jnp.where(ki <= qi, b, MASK_VALUE)
    biases()
    chips = [pl.multiple_of((b // 2) * CHIP, CHIP) for b in (ag.me, ag.xn, ag.yn, ag.dg)]
    gbd_ref[...] = jnp.zeros_like(gbd_ref)

    def act(i):
        rows = pl.ds(chips[i], CHIP)
        def body(n):
            cols = pl.ds(pl.multiple_of(n * 256, 256), 256)
            ga[rows, cols] = dot_nt(gyf[rows], wd[cols]).astype(BF)
        loop(0, 4, body)
        pltpu.make_async_copy(ga.at[rows], ga_out.at[rows], zs.at[i]).start()

    def colsum(n):
        part = pl.ds(pl.multiple_of(n * RB, RB), RB)
        gbd_ref[...] += jnp.sum(gyf[part].astype(F32), axis=0, keepdims=True)

    def weights():
        for l in loads[2:]:
            l.wait()
        def body(i):
            part = pl.ds(pl.multiple_of(i * CHIP, CHIP), CHIP)
            for t in range(3):
                for h in range(2):
                    w6[2 * t + h, part] = wq[part, t, h]
        loop(0, 4, body)
        pltpu.make_async_copy(w6, w6_out, ls.at[2]).start()
        gg.recv(6)
        act(0)

    def compute(idx, r0):
        rows = pl.ds(r0, CHIP)
        pltpu.make_async_copy(full.at[rows], h_out.at[rows], hs.at[idx]).start()
        def body(t):
            cols = pl.ds(pl.multiple_of(t * 256, 256), 256)
            w = jnp.concatenate([w6[2 * t], w6[2 * t + 1]], axis=1)
            qkv[rows, cols] = (dot(full[rows], w) + bq_ref[:, cols]).astype(BF)
        loop(0, 3, body)

    def start_gy():
        gg.send(1)
        gg.send(4)
        gg.recv(0)
        gg.send(5)
        gg.send(7)
        gg.recv(3)
        gg.send(2)
        gg.send(9)
    ag.run(compute, pre=weights, landed=start_gy)
    stores = [pltpu.make_async_copy(qkv, qkv_out, ls.at[0]), pltpu.make_async_copy(ctx, ctx_out, ls.at[1]),
              pltpu.make_async_copy(w6, w6_out, ls.at[2])]
    stores[0].start()

    def tile(block, n):
        cols = pl.ds(pl.multiple_of(n * TN, TN), TN)
        return dot(ctx[rows_at(block)], wo[:, cols])

    xb = lax.rem(ag.me // 2, 2)
    yb = ag.me // 4

    def attend(p):
        nx = xb + (1 - p // 2) * (1 - 2 * xb)
        ny = yb + (1 - lax.rem(p, 2)) * (1 - 2 * yb)
        i = 2 * ny + nx
        qrows = pl.ds(pl.multiple_of(i * CHIP, CHIP), CHIP)

        def one(h):
            lanes = [pl.ds(pl.multiple_of((2 * t + h) * 128, 128), 128) for t in range(3)]
            sl = slope(h)
            q = qkv[qrows, lanes[0]]
            ml[0:1] = jnp.full((1, CHIP), MASK_VALUE, F32)
            ml[1:2] = jnp.zeros((1, CHIP), F32)
            acc[...] = jnp.zeros_like(acc)
            def step(j, bias_ref):
                krows = pl.ds(pl.multiple_of(j * CHIP, CHIP), CHIP)
                s = dot_nt(qkv[krows, lanes[1]], q) * c1 + bias_ref[h]
                cj = sl * (j * CHIP).astype(F32)
                m = ml[0:1]
                mn = jnp.maximum(m, jnp.max(s, axis=0, keepdims=True) + cj)
                pr = jnp.exp2(s - (mn - cj))
                alpha = jnp.exp2(m - mn)
                ml[1:2] = ml[1:2] * alpha + jnp.sum(pr, axis=0, keepdims=True)
                ml[0:1] = mn
                acc[...] = acc[...] * alpha + dot_tn(qkv[krows, lanes[2]], pr.astype(BF))
            loop(0, i, lambda j: step(j, bias))
            step(i, biasm)
            ctx[qrows, lanes[0]] = jnp.transpose(acc[...] / ml[1:2]).astype(BF)
            lse_ref[h, :, qrows] = ml[0:1] + jnp.log(ml[1:2]) * LOG2E
        loop(0, 2, one)
        sc.give(p, tile, 2 * i + 1 - lax.rem(ag.me, 2))
    loop(0, 4, attend)
    stores[1].start()

    sc.keep(0, tile)
    sc.start(4, 7)
    sc.keep(1, tile)
    sc.start(5)
    sc.keep(2, tile)
    sc.start(8)
    sc.keep(3, tile)
    gg.recv(1)
    gg.send(8)
    gg.recv(4)
    gg.send(10)

    def keep_gy(i):
        rows = pl.ds(chips[i], CHIP)
        return pltpu.make_async_copy(gyf.at[rows], gy_out.at[rows], ys.at[i])
    keep_gy(0).start()
    gg.recv(7)
    gg.recv(8)
    keep_gy(1).start()
    act(1)
    gg.recv(5)
    gg.send(11)
    gg.recv(2)
    gg.send(12)
    gg.recv(9)
    gg.recv(10)
    keep_gy(2).start()
    act(2)
    gg.recv(11)
    gg.recv(12)
    keep_gy(3).start()
    sc.relays()
    act(3)
    loop(0, SEQ // RB, colsum)
    sc.arrive()

    def fin(rows):
        x1 = x[rows].astype(F32) + sc.total(rows) + bo_ref[...]
        x1_ref[rows] = x1
        gl_ref[rows] = norm_rows(x1, g2_ref[...], b2_ref[...]).astype(BF)
    row_blocks(fin)
    sc.finish()
    for k in range(13):
        gg.copy(k, gg.send_rows[k]).wait_send()
    for s in stores:
        s.wait()
    for i in range(4):
        rows = pl.ds(i * CHIP, CHIP)
        pltpu.make_async_copy(full.at[rows], h_out.at[rows], hs.at[i]).wait()
        pltpu.make_async_copy(ga.at[rows], ga_out.at[rows], zs.at[i]).wait()
        keep_gy(i).wait()


def mlp_kernel(g_hbm, gy_hbm, wu_hbm, bu_ref, ga_hbm, x1_hbm, g2_ref,
               r_out, gm_ref, gmb_ref, vec_ref, gwu_out, gwd_out, gbu_ref,
               full, ss, rs, gy, wu, x1, gp, r, gwu, gwd, ls, ys, *scratch):
    ag = Gather(full, ss, rs)
    sc = Scatter(*scratch)
    own = pltpu.make_async_copy(g_hbm, full.at[rows_at(ag.me)], ls.at[0])
    own.start()
    chips = [pl.multiple_of((b // 2) * CHIP, CHIP) for b in (ag.me, ag.xn, ag.yn, ag.dg)]
    load_wu = pltpu.make_async_copy(wu_hbm, wu, ls.at[2])
    load_ga = pltpu.make_async_copy(ga_hbm, gp, ls.at[1])
    load_gy = pltpu.make_async_copy(gy_hbm, gy, ys.at[0])
    load_x1 = pltpu.make_async_copy(x1_hbm, x1, ls.at[3])
    ag.barrier()
    own.wait()
    for k in (0, 3, 1, 4, 6):
        ag.send(k)
    load_wu.start()
    load_ga.start()
    gbu_ref[...] = jnp.zeros_like(gbu_ref)
    vec_ref[...] = jnp.zeros_like(vec_ref)
    load_gy.start()
    load_x1.start()

    k0 = math.sqrt(2.0 / math.pi)
    k1 = 0.044715

    def activation(z, grad):
        z2 = z * z
        t = jnp.tanh(k0 * (z + k1 * (z2 * z)))
        half = 0.5 * (1.0 + t)
        dz = half + (0.5 * z) * (1.0 - t * t) * (k0 * (1.0 + 3.0 * k1 * z2))
        return z * half, grad * dz

    def store_r(i):
        rows = pl.ds(chips[i], CHIP)
        return pltpu.make_async_copy(r.at[rows], r_out.at[rows], ys.at[i])

    def up(i):
        rows = pl.ds(chips[i], CHIP)
        def body(n):
            cols = pl.ds(pl.multiple_of(n * 256, 256), 256)
            act, gpre = activation(dot(full[rows], wu[:, cols]) + bu_ref[:, cols], gp[rows, cols].astype(F32))
            r[rows, cols] = act.astype(BF)
            gbu_ref[:, cols] += jnp.sum(gpre, axis=0, keepdims=True)
            gp[rows, cols] = gpre.astype(BF)
        loop(0, 4, body)
        store_r(i).start()

    def up_half(block, half):
        parts = [rows_at(block, half), rows_at(block + sc.delta, half)]
        def body(n):
            cols = pl.ds(pl.multiple_of(n * 256, 256), 256)
            lhs = jnp.concatenate([full[p] for p in parts], axis=0)
            grad = jnp.concatenate([gp[p, cols] for p in parts], axis=0)
            act, gpre = activation(dot(lhs, wu[:, cols]) + bu_ref[:, cols], grad.astype(F32))
            gbu_ref[:, cols] += jnp.sum(gpre, axis=0, keepdims=True)
            act, gpre = act.astype(BF), gpre.astype(BF)
            for k, p in enumerate(parts):
                r[p, cols] = act[k * 128:(k + 1) * 128]
                gp[p, cols] = gpre[k * 128:(k + 1) * 128]
        loop(0, 4, body)

    def tile(block, n):
        cols = pl.ds(pl.multiple_of(n * TN, TN), TN)
        return dot_nt(gp[rows_at(block)], wu[cols])

    load_wu.wait()
    load_ga.wait()
    load_gy.wait()
    ag.recv(6)
    up(0)
    ag.recv(0)
    ag.send(5)
    ag.send(7)
    ag.recv(3)
    ag.send(2)
    ag.send(9)
    ag.recv(7)
    up_half(ag.xn, 0)
    ag.recv(9)
    up_half(ag.yn, 1)
    ag.recv(1)
    ag.send(8)
    ag.recv(4)
    ag.send(10)
    ag.recv(8)
    up_half(ag.xn, 1)
    store_r(1).start()
    sc.give(1, tile)
    ag.recv(10)
    up_half(ag.yn, 0)
    store_r(2).start()
    sc.keep(1, tile)
    sc.start(5)
    sc.give(2, tile)
    ag.recv(5)
    ag.send(11)
    ag.recv(2)
    ag.send(12)
    sc.keep(2, tile)
    sc.start(8)
    ag.recv(11)
    ag.recv(12)
    up(3)
    sc.give(0, tile)
    sc.give(3, tile)
    sc.keep(0, tile)
    sc.start(4, 7)
    sc.keep(3, tile)

    def gwu_step(i):
        cols = pl.ds(pl.multiple_of(i * 256, 256), 256)
        gwu[cols] = dot_tn(full[:, cols], gp[...]).astype(BF)
        pltpu.make_async_copy(gwu.at[cols], gwu_out.at[cols], ls.at[4]).start()

    def gwd_step(i):
        cols = pl.ds(pl.multiple_of(i * 256, 256), 256)
        gwd[cols] = dot_tn(r[:, cols], gy[...]).astype(BF)
        pltpu.make_async_copy(gwd.at[cols], gwd_out.at[cols], ls.at[5]).start()

    loop(0, 7, gwu_step)
    sc.relays()
    loop(7, 8, gwu_step)
    loop(0, 4, gwd_step)
    load_x1.wait()
    sc.arrive()

    def fin(rows):
        ct = sc.total(rows)
        dx, xhat = norm_rows_back(x1[rows], g2_ref[...], ct)
        mine = pl.ds(pl.multiple_of(ag.me * ROWS + rows.start, RB), RB)
        gm = gy[mine].astype(F32) + dx
        gm_ref[rows] = gm
        gmb_ref[rows] = gm.astype(BF)
        vec_ref[0:1] += jnp.sum(ct * xhat, axis=0, keepdims=True)
        vec_ref[1:2] += jnp.sum(ct, axis=0, keepdims=True)
        vec_ref[2:3] += jnp.sum(gm, axis=0, keepdims=True)
    row_blocks(fin)
    for k in range(13):
        ag.copy(k, ag.send_rows[k]).wait_send()
    sc.finish()
    for i in range(4):
        rows = pl.ds(chips[i], CHIP)
        pltpu.make_async_copy(r.at[rows], r_out.at[rows], ys.at[i]).wait()
    pltpu.make_async_copy(gwu, gwu_out, ls.at[4]).wait()
    pltpu.make_async_copy(gwd, gwd_out, ls.at[5]).wait()


def tail_kernel(sl_ref, gm_hbm, wo_hbm, r_hbm, wd_hbm, qkv_hbm, ctx_hbm, lse_ref, w6_hbm, x_hbm, gmf_hbm, x1_hbm, bd_ref, g1_ref,
                h_hbm, vec2_ref, y_ref, gx_ref, vec_out, gwq_out, gwo_out, gb_ref,
                full, ss, rs, wo, r, wd, qkv, ctx, w6, x1, gc, gq, gwq, gwo, bias, biasm, delta, dqt, dk, dv, vec, bufv,
                ls, vs, vr, pb, din1, rel1, fin1, ss1, rs1, din2, rel2, fin2, ss2, rs2):
    ag = Gather(full, ss, rs)
    s1 = Scatter(pb, din1, rel1, fin1, ss1, rs1)
    s2 = Scatter(pb, din2, rel2, fin2, ss2, rs2)
    pairs = [(gm_hbm, full.at[rows_at(ag.me)]), (wd_hbm, wd), (r_hbm, r), (wo_hbm, wo), (qkv_hbm, qkv), (ctx_hbm, ctx), (w6_hbm, w6),
             (x1_hbm, x1)]
    loads = [pltpu.make_async_copy(src, dst, ls.at[i]) for i, (src, dst) in enumerate(pairs)]
    loads[0].start()
    peers = [lax.rem(ag.me + k, 8) for k in range(1, 8)]
    entry_barrier(peers)
    loads[0].wait()
    for k in (0, 3, 1, 4, 6):
        ag.send(k)
    for l in loads[1:]:
        l.start()
    scale = 128 ** -0.5
    c1 = scale * LOG2E
    vec[...] = vec2_ref[...]
    gb_ref[...] = jnp.zeros_like(gb_ref)

    def mtile(block, n):
        cols = pl.ds(pl.multiple_of(n * TN, TN), TN)
        return dot(r[rows_at(block)], wd[:, cols])

    def gcs(block):
        rows = pl.ds(pl.multiple_of((block // 2) * CHIP, CHIP), CHIP)
        gc[rows] = dot_nt(full[rows], wo[...]).astype(BF)

    loads[1].wait()
    loads[2].wait()
    for d in range(4):
        s1.give(d, mtile)
    s1.keep(0, mtile)
    loads[3].wait()
    ag.recv(6)
    gcs(ag.me)
    ag.recv(0)
    ag.send(5)
    ag.send(7)
    ag.recv(3)
    ag.send(2)
    ag.send(9)
    for d in range(1, 4):
        s1.keep(d, mtile)
    load_h = [pltpu.make_async_copy(h_hbm.at[:, pl.ds(i * 1024, 1024)], r, ls.at[10 + i]) for i in range(2)]
    load_h[0].start()
    for l in loads[4:]:
        l.wait()

    def rowsum(i):
        rows = pl.ds(pl.multiple_of(i * CHIP, CHIP), CHIP)
        for h in range(2):
            lanes = pl.ds(h * 128, 128)
            prod = gc[rows, lanes].astype(F32) * ctx[rows, lanes].astype(F32)
            delta[h:h + 1, rows] = jnp.sum(jnp.transpose(prod), axis=0, keepdims=True)

    ag.recv(1)
    ag.send(8)
    ag.recv(4)
    ag.send(10)
    ag.recv(7)
    ag.recv(8)
    gcs(ag.xn)
    ag.recv(9)
    ag.recv(10)
    gcs(ag.yn)
    ag.recv(5)
    ag.send(11)
    ag.recv(2)
    ag.send(12)
    s1.start(4, 7, 5, 8)
    ag.recv(11)
    ag.recv(12)
    gcs(ag.dg)
    x = wo
    load_x = pltpu.make_async_copy(x_hbm, x, ls.at[8])
    load_x.start()
    loop(0, SEQ // CHIP, rowsum)

    def put(h, t, rows, val):
        val = val.astype(BF)
        gq[rows, (2 * t + h) * 128:(2 * t + h + 1) * 128] = val
        gb_ref[t, h:h + 1] += jnp.sum(val.astype(F32), axis=0, keepdims=True)

    def head(h):
        sl = sl_ref[2 * ag.me + h] * LOG2E
        ki = lax.broadcasted_iota(jnp.int32, (CHIP, CHIP), 0)
        qi = lax.broadcasted_iota(jnp.int32, (CHIP, CHIP), 1)
        b = ki.astype(F32) * sl
        bias[...] = b
        biasm[...] = jnp.where(ki <= qi, b, MASK_VALUE)
        dqt[...] = jnp.zeros_like(dqt)
        lq, lk, lv, lo = (pl.ds((2 * t + h) * 128, 128) for t in (0, 1, 2, 0))

        def kblock(j):
            krows = pl.ds(pl.multiple_of(j * CHIP, CHIP), CHIP)
            k = qkv[krows, lk]
            v = qkv[krows, lv]
            dk[...] = jnp.zeros_like(dk)
            dv[...] = jnp.zeros_like(dv)
            cj = sl * (j * CHIP).astype(F32)
            def step(i, bias_ref):
                qrows = pl.ds(pl.multiple_of(i * CHIP, CHIP), CHIP)
                q = qkv[qrows, lq]
                do = gc[qrows, lo]
                p = jnp.exp2(dot_nt(k, q) * c1 + bias_ref[...] - (lse_ref[h, :, qrows] - cj))
                dv[...] += dot(p.astype(BF), do)
                ds = (p * (dot_nt(v, do) - delta[h:h + 1, qrows])).astype(BF)
                dk[...] += dot(ds, q)
                dqt[:, qrows] += dot_tn(k, ds)
            step(j, biasm)
            loop(j + 1, SEQ // CHIP, lambda i: step(i, bias))
            put(h, 1, krows, dk[...] * scale)
            put(h, 2, krows, dv[...])
        loop(0, SEQ // CHIP, kblock)

        def qout(i):
            rows = pl.ds(pl.multiple_of(i * CHIP, CHIP), CHIP)
            put(h, 0, rows, jnp.transpose(dqt[:, rows]) * scale)
        loop(0, SEQ // CHIP, qout)

    head(0)
    s1.relays()
    head(1)

    def htile(block, n):
        rows = rows_at(block)
        cols = pl.ds(pl.multiple_of(n * TN, TN), TN)
        out = None
        for t in range(3):
            w = jnp.concatenate([w6[2 * t, cols], w6[2 * t + 1, cols]], axis=1)
            part = dot_nt(gq[rows, t * 256:(t + 1) * 256], w)
            out = part if out is None else out + part
        return out

    for k in range(4):
        s1.copy(k).wait_send()
    s2.run(htile)

    stores = [pltpu.make_async_copy(gwq, gwq_out.at[pl.ds(i * 1024, 1024)], ls.at[12]) for i in range(2)]
    stores.append(pltpu.make_async_copy(gwo, gwo_out, ls.at[13]))

    def wq():
        def body(i):
            src = pl.ds(pl.multiple_of(i * 256, 256), 256)
            val = dot_tn(r[:, src], gq[...])
            for t in range(3):
                pair = [val[:, (2 * t + h) * 128:(2 * t + h + 1) * 128] for h in range(2)]
                gwq[src, t] = jnp.stack(pair, axis=1).astype(BF)
        return body

    load_h[0].wait()
    loop(0, 4, wq())
    load_h[1].start()
    stores[0].start()
    s2.relays()
    s1.arrive()

    def yrow(rows):
        y_ref[rows] = (x1[rows] + s1.total(rows) + bd_ref[...]).astype(BF)
    row_blocks(yrow)
    gm = x1
    load_gm = pltpu.make_async_copy(gmf_hbm, gm, ls.at[9])
    load_gm.start()

    def wout(n):
        cols = pl.ds(pl.multiple_of(n * TN, TN), TN)
        gwo[:, cols] = dot_tn(ctx[...], full[:, cols]).astype(BF)
    loop(0, D // TN, wout)
    stores[2].start()
    load_h[1].wait()
    stores[0].wait()
    loop(0, 4, wq())
    stores[1].start()
    load_x.wait()
    load_gm.wait()
    s2.arrive()

    def fin(rows):
        ct = s2.total(rows)
        dx, xhat = norm_rows_back(x[rows].astype(F32), g1_ref[...], ct)
        gx_ref[rows] = (gm[rows] + dx).astype(BF)
        vec[3:4] += jnp.sum(ct * xhat, axis=0, keepdims=True)
        vec[4:5] += jnp.sum(ct, axis=0, keepdims=True)
    row_blocks(fin)
    s1.finish(4)
    s2.finish()
    copies = [pltpu.make_async_remote_copy(src_ref=vec, dst_ref=bufv.at[ag.me], send_sem=vs.at[k], recv_sem=vr.at[k],
                                           device_id={'tp': peers[k]}, device_id_type=MESH) for k in range(7)]
    for c in copies:
        c.start()
    bufv[ag.me] = vec[...]
    for k in range(13):
        ag.copy(k, ag.send_rows[k]).wait_send()
    for s in stores[1:]:
        s.wait()
    for c in copies:
        c.wait()
    total = bufv[0]
    for i in range(1, 8):
        total = total + bufv[i]
    vec_out[...] = total


def finish_kernel(y, gx, wo, wq, wu, wd, vec, bu, bd, bq, y_out, gx_out, wo_out, wq_out, wu_out, wd_out,
                  v0, v1, v2, v3, v4, bu_out, bd_out, bq_out, *scratch):
    bufs, si, so = scratch[:6], scratch[6], scratch[7]
    parts = []
    for src, dst, buf, size, n in ((wu, wu_out, bufs[4], 512, 4), (wd, wd_out, bufs[5], 256, 4), (wq, wq_out, bufs[3], 512, 4),
                                   (y, y_out, bufs[0], 256, 1), (gx, gx_out, bufs[1], 256, 1), (wo, wo_out, bufs[2], 256, 1)):
        for i in range(n):
            rows = pl.ds(i * size, size)
            k = len(parts)
            parts.append((pltpu.make_async_copy(src.at[rows], buf.at[rows], si.at[k]),
                          pltpu.make_async_copy(buf.at[rows], dst.at[rows], so.at[k])))
    for load, _ in parts:
        load.start()
    for i, out in enumerate((v0, v1, v2, v3, v4)):
        out[...] = vec[i:i + 1]
    bu_out[...] = bu[...]
    bd_out[...] = bd[...]
    bq_out[...] = bq[...]
    for load, store in parts:
        load.wait()
        store.start()
    for _, store in parts:
        store.wait()


def finish(big, small):
    row = jax.ShapeDtypeStruct((1, D), F32)
    like = [jax.ShapeDtypeStruct(v.shape, v.dtype) for v in (*big, *small)]
    return pl.pallas_call(
        finish_kernel,
        name='finish',
        out_shape=like[:6] + [row] * 5 + like[7:],
        in_specs=[HB] * 6 + [VM] * 4,
        out_specs=[HB] * 6 + [VM] * 8,
        scratch_shapes=[pltpu.VMEM(v.shape, BF) for v in big] + [pltpu.SemaphoreType.DMA((15,))] * 2,
    )(*big, *small)


def solution(mesh):
    def local_step(x, ln1_gamma, ln1_beta, w_qkv, b_qkv, w_out, b_out, ln2_gamma, ln2_beta, w_up, b_up, w_down, b_down, grad_y):
        slopes = alibi_slopes(16)
        row = lambda v: v.reshape(1, -1)
        x2, gy2 = x[0], grad_y[0]
        bq = b_qkv.transpose(1, 0, 2).reshape(1, 768)

        qkv, ctx, lse, h_full, gy_full, x1, g_loc, w6, ga, gbd = call(
            front_kernel, 'front', 0, [pl.BlockSpec(memory_space=pltpu.SMEM), HB, VM, VM, HB, VM, HB, HB, VM, VM, VM, HB],
            [((SEQ, 768), BF, HB), ((SEQ, 256), BF, HB), ((2, 1, SEQ), F32, VM), ((SEQ, D), BF, HB), ((SEQ, D), BF, HB),
             ((ROWS, D), F32, VM), ((ROWS, D), BF, VM), ((6, D, 128), BF, HB), ((SEQ, 1024), BF, HB), ((1, D), F32, VM)],
            GATHER_SCRATCH * 2 + [pltpu.VMEM((ROWS, D), BF), pltpu.VMEM((6, D, 128), BF), pltpu.VMEM((256, D), BF),
                                  pltpu.VMEM((SEQ, 768), BF), pltpu.VMEM((SEQ, 256), BF), pltpu.VMEM((2, CHIP, CHIP), F32),
                                  pltpu.VMEM((2, CHIP, CHIP), F32), pltpu.VMEM((128, CHIP), F32), pltpu.VMEM((8, CHIP), F32),
                                  pltpu.VMEM((D, 3, 2, 128), BF), pltpu.VMEM((1024, D), BF), pltpu.VMEM((SEQ, 1024), BF),
                                  pltpu.SemaphoreType.DMA((5,))] + [pltpu.SemaphoreType.DMA((4,))] * 3
            + SCATTER_SCRATCH,
            (slopes, x2, row(ln1_gamma), row(ln1_beta), w_qkv.transpose(0, 2, 1, 3), bq, gy2, w_out, row(b_out), row(ln2_gamma),
             row(ln2_beta), w_down), 20 << 30)
        r, gm, gm_bf, vec2, g_wu, g_wd, gbu = call(
            mlp_kernel, 'mlp', 2, [HB, HB, HB, VM, HB, HB, VM],
            [((SEQ, 1024), BF, HB), ((ROWS, D), F32, VM), ((ROWS, D), BF, VM), ((8, D), F32, VM), ((D, 1024), BF, HB),
             ((1024, D), BF, HB), ((1, 1024), F32, VM)],
            GATHER_SCRATCH + [pltpu.VMEM((SEQ, D), BF), pltpu.VMEM((D, 1024), BF), pltpu.VMEM((ROWS, D), F32),
                              pltpu.VMEM((SEQ, 1024), BF), pltpu.VMEM((SEQ, 1024), BF), pltpu.VMEM((D, 1024), BF),
                              pltpu.VMEM((1024, D), BF), pltpu.SemaphoreType.DMA((6,)), pltpu.SemaphoreType.DMA((4,))] + SCATTER_SCRATCH,
            (g_loc, gy_full, w_up, row(b_up), ga, x1, row(ln2_gamma)), 36 << 30)
        y, g_x, vec, g_wq, g_wo, g_bq = call(
            tail_kernel, 'tail', 3, [pl.BlockSpec(memory_space=pltpu.SMEM)] + [HB] * 6 + [VM] + [HB] * 4 + [VM] * 2 + [HB, VM],
            [((ROWS, D), BF, VM), ((ROWS, D), BF, VM), ((8, D), F32, VM), ((D, 3, 2, 128), BF, HB), ((256, D), BF, HB), ((3, 2, 128), F32, VM)],
            GATHER_SCRATCH + [pltpu.VMEM((256, D), BF), pltpu.VMEM((SEQ, 1024), BF), pltpu.VMEM((1024, D), BF), pltpu.VMEM((SEQ, 768), BF),
                              pltpu.VMEM((SEQ, 256), BF), pltpu.VMEM((6, D, 128), BF), pltpu.VMEM((ROWS, D), F32),
                              pltpu.VMEM((SEQ, 256), BF), pltpu.VMEM((SEQ, 768), BF), pltpu.VMEM((1024, 3, 2, 128), BF),
                              pltpu.VMEM((256, D), BF), pltpu.VMEM((CHIP, CHIP), F32), pltpu.VMEM((CHIP, CHIP), F32),
                              pltpu.VMEM((2, SEQ), F32), pltpu.VMEM((128, SEQ), F32), pltpu.VMEM((CHIP, 128), F32),
                              pltpu.VMEM((CHIP, 128), F32), pltpu.VMEM((8, D), F32), pltpu.VMEM((8, 8, D), F32),
                              pltpu.SemaphoreType.DMA((14,)), pltpu.SemaphoreType.DMA((7,)), pltpu.SemaphoreType.DMA((7,))]
            + SCATTER_SCRATCH + SCATTER_REST,
            (slopes, gm_bf, w_out, r, w_down, qkv, ctx, lse, w6, x2, gm, x1, row(b_down), row(ln1_gamma), h_full, vec2), 55 << 30)
        y, g_x, g_wo, g_wq, g_wu, g_wd, g_g2, g_b2, g_bo, g_g1, g_b1, gbu, gbd, g_bq = finish(
            (y, g_x, g_wo, g_wq, g_wu, g_wd), (vec, gbu, gbd, g_bq))
        g_wq, g_bq = g_wq.transpose(0, 2, 1, 3), g_bq.transpose(1, 0, 2)
        return (y[None], g_x[None], g_g1[0], g_b1[0], g_wq, g_bq, g_wo, g_bo[0], g_g2[0], g_b2[0], g_wu, gbu[0], g_wd, gbd[0])

    row_spec = P('dp', 'tp', None)
    in_specs = (row_spec, P(), P(), P(None, 'tp', None, None), P('tp', None, None), P('tp', None), P(), P(), P(),
                P(None, 'tp'), P('tp'), P('tp', None), P(), row_spec)
    out_specs = (row_spec, row_spec, P('dp'), P('dp'), P('dp', 'tp', None, None), P(('dp', 'tp'), None, None),
                 P(('dp', 'tp'), None), P('dp'), P('dp'), P('dp'), P('dp', 'tp'), P(('dp', 'tp')), P(('dp', 'tp'), None), P('dp'))
    return jax.shard_map(local_step, mesh=mesh, in_specs=in_specs, out_specs=out_specs, check_vma=False)
```
